32 devices in a mesh: rep: 1, dp: 32 (over x, y, z, core).
Axes of the slice: x: 2, y: 2, z: 4, core: 2. Of those that a mesh axis runs over, the one named last changes fastest.
Arguments:
- x: bfloat16 [32, 2048, 1024], P(('rep', 'dp'))
- dy: bfloat16 [32, 2048, 1024], P(('rep', 'dp'))
- w_gate: bfloat16 [2, 1024, 4096], P(None, 'dp')
- w_up: bfloat16 [2, 1024, 4096], P(None, 'dp')
- w_down: bfloat16 [2, 4096, 1024], P(None, 'dp')
- m_w_gate: float32 [2, 1024, 4096], P(None, 'dp')
- m_w_up: float32 [2, 1024, 4096], P(None, 'dp')
- m_w_down: float32 [2, 4096, 1024], P(None, 'dp')
- v_w_gate: float32 [2, 1024, 4096], P(None, 'dp')
- v_w_up: float32 [2, 1024, 4096], P(None, 'dp')
- v_w_down: float32 [2, 4096, 1024], P(None, 'dp')
Outputs:
- output 1: bfloat16 [2, 1024, 4096], P('rep', 'dp')
- output 2: bfloat16 [2, 1024, 4096], P('rep', 'dp')
- output 3: bfloat16 [2, 4096, 1024], P('rep', 'dp')
- output 4: float32 [2, 1024, 4096], P('rep', 'dp')
- output 5: float32 [2, 1024, 4096], P('rep', 'dp')
- output 6: float32 [2, 4096, 1024], P('rep', 'dp')
- output 7: float32 [2, 1024, 4096], P('rep', 'dp')
- output 8: float32 [2, 1024, 4096], P('rep', 'dp')
- output 9: float32 [2, 4096, 1024], P('rep', 'dp')
All inputs are finite; a program needn't handle non-finite values.
Results may differ from the reference program's by a relative error of at most 0.0278.
Values are sent between devices in bfloat16 or wider.
A program may use at most 2 GiB of HBM per device.

```python
import jax
import jax.numpy as jnp
from jax import lax

SEQUENCES = 32
TOKENS = 2048
D = 1024
FF = 4096
LAYERS = 2
NAMES = ("w_gate", "w_up", "w_down")
SHAPES = {"w_gate": (LAYERS, D, FF), "w_up": (LAYERS, D, FF), "w_down": (LAYERS, FF, D)}


def bump(key, n, height):
    away = (jnp.arange(n, dtype=jnp.int32) - jax.random.randint(key, (), 0, n, jnp.int32)) % n
    return jnp.where(away < n // 8, height, 1.0)


def together(key, own, strength):
    shared = jax.random.normal(key, own.shape[1:], jnp.float32)
    return (own + strength * shared) * lax.rsqrt(1 + strength * strength)


def setup_inputs(seed: int = 0, part: int = 0) -> dict:
    kx, kdy, ka, kb, kz, kf, kh, kl, *keys = jax.random.split(jax.random.key(seed), 8 + 3 * len(NAMES))
    kx, kdy, ka, kb = (jax.random.fold_in(k, part) for k in (kx, kdy, ka, kb))
    kw, km, kv = (keys[i::3] for i in range(3))
    shape = (SEQUENCES, TOKENS, D)
    much_x, much_dy = jax.random.uniform(kz, (2,), jnp.float32, 0.0, 1.0)
    loud = 2.0 ** jax.random.uniform(jax.random.fold_in(kz, 1), (), jnp.float32, -1.0, 2.0)
    layers = 2.0 ** jax.random.uniform(kl, (LAYERS, 1, 1), jnp.float32, -1.0, 1.0)
    x = together(ka, jax.random.normal(kx, shape, jnp.float32), much_x) * bump(kf, D, 4.0)
    dy = together(kb, jax.random.normal(kdy, shape, jnp.float32), much_dy)
    drawn = {"x": x.astype(jnp.bfloat16), "dy": (loud * dy * (SEQUENCES * TOKENS) ** -0.5).astype(jnp.bfloat16)}
    for key, name in zip(kw, NAMES, strict=True):
        w = jax.random.normal(key, SHAPES[name], jnp.float32) * SHAPES[name][1] ** -0.5
        drawn[name] = (w * {"w_gate": 1.0, "w_up": bump(kh, FF, 4.0), "w_down": layers}[name]).astype(jnp.bfloat16)
    for key, name in zip(km, NAMES, strict=True):
        drawn[f"m_{name}"] = 0.1 * jax.random.normal(key, SHAPES[name], jnp.float32)
    for key, name in zip(kv, NAMES, strict=True):
        drawn[f"v_{name}"] = jax.random.uniform(key, SHAPES[name], jnp.float32, 0.005, 0.015)
    return drawn


def matmul(a, w):
    return jnp.dot(a, w, preferred_element_type=jnp.float32).astype(jnp.bfloat16)


def normed(h):
    wide = h.astype(jnp.float32)
    scale = lax.rsqrt(jnp.mean(wide**2, -1, keepdims=True) + 1e-6)
    return (wide * scale).astype(jnp.bfloat16)


def layer(h, w):
    a = normed(h)
    gate = jnp.dot(a, w["w_gate"], preferred_element_type=jnp.float32)
    up = jnp.dot(a, w["w_up"], preferred_element_type=jnp.float32)
    return h + matmul((jax.nn.silu(gate) * up).astype(jnp.bfloat16), w["w_down"])


def adamw(w, m, v, g):
    m = 0.9 * m + 0.1 * g
    v = 0.95 * v + 0.05 * g * g
    step = m * lax.rsqrt(v + 1e-8) + 0.1 * w
    return (w - 0.02 * step).astype(jnp.bfloat16), m, v


def clipped(gradients, sum_of_squares, count):
    factor = jnp.minimum(1.0, 0.5 * lax.rsqrt(sum_of_squares / count + 1e-30))
    return [g * factor for g in gradients]


def stack(weights, h):
    return lax.scan(lambda h, w: (layer(h, w), None), h, weights)[0]


def reference(x, dy, w_gate, w_up, w_down, m_w_gate, m_w_up, m_w_down, v_w_gate, v_w_up, v_w_down):
    weights = dict(zip(NAMES, (w_gate, w_up, w_down), strict=True))

    def take(so_far, sequence):
        h, by_y = sequence
        _, back = jax.vjp(lambda w: stack(w, h), weights)
        return jax.tree.map(lambda total, term: total + term.astype(jnp.float32), so_far, back(by_y)[0]), None

    none_yet = {name: jnp.zeros(w.shape, jnp.float32) for name, w in weights.items()}
    by_weights, _ = lax.scan(take, none_yet, (x, dy))
    gradients = [by_weights[name].astype(jnp.bfloat16).astype(jnp.float32) for name in NAMES]
    gradients = clipped(gradients, sum(jnp.sum(g * g) for g in gradients), sum(g.size for g in gradients))
    new = [
        adamw(w.astype(jnp.float32), m, v, g)
        for w, m, v, g in zip((w_gate, w_up, w_down), (m_w_gate, m_w_up, m_w_down), (v_w_gate, v_w_up, v_w_down), gradients, strict=True)
    ]
    return tuple(one[which] for which in range(3) for one in new)
```

```python
import functools

import jax
import jax.numpy as jnp
from jax import lax
from jax.experimental import pallas as pl
from jax.experimental.pallas import tpu as pltpu
from jax.sharding import PartitionSpec as P

NAMES = ("w_gate", "w_up", "w_down")
BF, F32 = jnp.bfloat16, jnp.float32
MESH = pl.DeviceIdType.MESH
CHUNKS = 24
SLOTS = 8


def matmul(a, w):
    return jnp.dot(a, w, preferred_element_type=jnp.float32).astype(jnp.bfloat16)


def normed(h):
    wide = h.astype(jnp.float32)
    scale = lax.rsqrt(jnp.mean(wide**2, -1, keepdims=True) + 1e-6)
    return (wide * scale).astype(jnp.bfloat16)


def layer(h, w):
    a = normed(h)
    gate = jnp.dot(a, w["w_gate"], preferred_element_type=jnp.float32)
    up = jnp.dot(a, w["w_up"], preferred_element_type=jnp.float32)
    return h + matmul((jax.nn.silu(gate) * up).astype(jnp.bfloat16), w["w_down"])


def adamw(w, m, v, g):
    m = 0.9 * m + 0.1 * g
    v = 0.95 * v + 0.05 * g * g
    step = m * lax.rsqrt(v + 1e-8) + 0.1 * w
    return (w - 0.02 * step).astype(jnp.bfloat16), m, v


def place():
    me = lax.axis_index("dp")
    return me // 16, (me // 8) % 2, (me // 2) % 4, me % 2


def number(x, y, z, c):
    return ((x * 2 + y) * 4 + z) * 2 + c


def greet():
    x, y, z, c = place()
    barrier = pltpu.get_barrier_semaphore()
    others = [(1 - x, y, z, c), (x, 1 - y, z, c), (x, y, z, 1 - c)]
    others += [(x, y, (z + hop) % 4, c) for hop in (1, 2, 3)]
    for other in others:
        pl.semaphore_signal(barrier, 1, device_id={"dp": number(*other)}, device_id_type=MESH)
    pl.semaphore_wait(barrier, len(others))


def send(src, dst, sems, where):
    return pltpu.make_async_remote_copy(
        src_ref=src, dst_ref=dst, send_sem=sems[0], recv_sem=sems[1], device_id={"dp": number(*where)}, device_id_type=MESH
    )


def gather_chunks():
    order = []
    for layer_number in range(2):
        first = 3 * layer_number
        order += [(first + i, 1024 * q, 1024) for q in range(4) for i in (0, 1)]
        order += [(first + 2, 256 * q, 256) for q in range(4)]
    return order


GATHER_AT = (0, 2, 4, 6, 8)


def gather_kernel(*refs):
    shards, whole = refs[0:6], refs[6:12]
    mine, sems, local = refs[12:18], refs[18], refs[19]
    x, y, z, c = place()
    for i in range(6):
        pltpu.make_async_copy(shards[i], mine[i], local.at[i]).start()
    greet()
    chunks = gather_chunks()

    def copies(k, stage):
        i, first, columns = chunks[k]
        cut = pl.ds(first, columns)
        full = whole[i]

        def pair(n):
            return sems.at[0, k, n], sems.at[1, k, n]

        near = (x, 1 - y, z, c) if k % 2 == 0 else (1 - x, y, z, c)
        far = (1 - x, y, z, c) if k % 2 == 0 else (x, 1 - y, z, c)
        twin = (x, y, z, 1 - c)
        if stage == 0:
            own = full.at[x, y, z, c, :, cut]
            return [lambda hop=hop: send(shards[i].at[:, cut], own, pair(hop - 1), (x, y, (z + hop) % 4, c)) for hop in (1, 2, 3)]
        if stage == 1:
            part = full.at[x, y, :, c, :, cut]
            return [lambda: send(part, part, pair(3), near), lambda: send(part, part, pair(4), twin)]
        if stage == 2:
            part = full.at[x, :, :, c, :, cut] if k % 2 == 0 else full.at[:, y, :, c, :, cut]
            late = full.at[x, 1 - y, :, c, :, cut] if k % 2 == 0 else full.at[1 - x, y, :, c, :, cut]
            return [lambda: send(part, part, pair(5), far), lambda: send(late, late, pair(6), twin)]
        part = full.at[1 - x, :, :, c, :, cut] if k % 2 == 0 else full.at[:, 1 - y, :, c, :, cut]
        return [lambda: send(part, part, pair(7), twin)]

    for i in range(6):
        pltpu.make_async_copy(shards[i], mine[i], local.at[i]).wait()
        pltpu.make_async_copy(mine[i], whole[i].at[x, y, z, c], local.at[i]).start()
    for t in range(CHUNKS + GATHER_AT[-1]):
        if t == 2:
            for i in range(6):
                pltpu.make_async_copy(mine[i], whole[i].at[x, y, z, c], local.at[i]).wait()
        for stage in (4, 3, 2, 1, 0):
            k = t - GATHER_AT[stage]
            if not 0 <= k < CHUNKS:
                continue
            if stage in (1, 2, 3):
                for copy in copies(k, stage - 1)[: 3 if stage == 1 else 1]:
                    copy().wait_recv()
            if stage == 4:
                for copy in copies(k, 1)[1:] + copies(k, 2)[1:] + copies(k, 3):
                    copy().wait_recv()
                for past in range(4):
                    for copy in copies(k, past):
                        copy().wait_send()
            else:
                for copy in copies(k, stage):
                    copy().start()


def gathered(weights):
    shards = [w[n] for n in range(2) for w in weights]
    tall = [s.shape for s in shards]
    return pl.pallas_call(
        gather_kernel,
        name="gather",
        out_shape=[jax.ShapeDtypeStruct((2, 2, 4, 2) + s, BF) for s in tall],
        in_specs=[pl.BlockSpec(memory_space=pl.ANY)] * 6,
        out_specs=[pl.BlockSpec(memory_space=pl.ANY)] * 6,
        scratch_shapes=[pltpu.VMEM(s, BF) for s in tall]
        + [pltpu.SemaphoreType.DMA((2, CHUNKS, 8)), pltpu.SemaphoreType.DMA((6,))],
        compiler_params=pltpu.CompilerParams(collective_id=0, has_side_effects=True),
    )(*shards)


SUM_AT = (0, 1, 3, 5, 6)


def wide(ref, *at):
    return ref[at].astype(F32)


def sum_stages(k, own, fromtwin, fromfar, fromnear, fromz, sems, out, squares):
    x, y, z, c = place()
    slot, color = k % SLOTS, k % 2
    f, n = x + color * (y - x), y + color * (x - y)
    far = (x + (1 - color) * (1 - 2 * x), y + color * (1 - 2 * y), z, c)
    near = (x + color * (1 - 2 * x), y + (1 - color) * (1 - 2 * y), z, c)

    def pair(i):
        return sems.at[0, slot, i], sems.at[1, slot, i]

    def to_twin():
        return send(own.at[SLOTS + k % 2], fromtwin.at[slot], pair(0), (x, y, z, 1 - c))

    def to_far():
        return send(fromtwin.at[slot, pl.ds((1 - f) * 8, 8)], fromfar.at[slot], pair(1), far)

    def to_near():
        return send(fromtwin.at[slot, pl.ds(f * 8 + (1 - n) * 4, 4)], fromnear.at[slot], pair(2), near)

    base = f * 8 + n * 4

    def to_z(hop):
        to = (z + hop) % 4
        return send(fromtwin.at[slot, base + to], fromz.at[slot, hop - 1], pair(2 + hop), (x, y, to, c))

    def first():
        to_twin().start()

    def second():
        to_twin().wait()

        def add(i, _):
            p = (1 - f) * 8 + i
            fromtwin[slot, p] = (wide(own, slot, p) + wide(fromtwin, slot, p)).astype(BF)
            return 0

        lax.fori_loop(0, 8, add, 0)
        to_far().start()

    def third():
        to_far().wait_recv()

        def add(i, _):
            q = (1 - n) * 4 + i
            p = f * 8 + q
            fromtwin[slot, p] = (wide(own, slot, p) + wide(fromtwin, slot, p) + wide(fromfar, slot, q)).astype(BF)
            return 0

        lax.fori_loop(0, 4, add, 0)
        to_near().start()

    def fourth():
        to_near().wait_recv()
        for hop in (1, 2, 3):
            to = (z + hop) % 4
            p, q = base + to, n * 4 + to
            total = wide(own, slot, p) + wide(fromtwin, slot, p) + wide(fromfar, slot, q) + wide(fromnear, slot, to)
            fromtwin[slot, p] = total.astype(BF)
            to_z(hop).start()

    def fifth():
        for hop in (1, 2, 3):
            to_z(hop).wait()
        to_far().wait_send()
        to_near().wait_send()
        p, q = base + z, n * 4 + z
        total = wide(own, slot, p) + wide(fromtwin, slot, p) + wide(fromfar, slot, q) + wide(fromnear, slot, z)
        total = (total + wide(fromz, slot, 0) + wide(fromz, slot, 1) + wide(fromz, slot, 2)).astype(BF)
        out[k] = total
        square = total.astype(F32)
        square = square * square
        squares[...] += jnp.sum(square.reshape(16, 8, 256), axis=0)

    return first, second, third, fourth, fifth


def sum_tick(t, bufs):
    for stage in (4, 3, 2, 1, 0):
        k = t - SUM_AT[stage]

        @pl.when(jnp.logical_and(k >= 0, k < CHUNKS))
        def _():
            sum_stages(k, *bufs)[stage]()


def all_squares(squares, total, box, sems):
    x, y, z, c = place()
    box[0] = jnp.broadcast_to(jnp.sum(squares[...]), (8, 128))
    for i, other in enumerate([(x, y, z, 1 - c), (1 - x, y, z, c), (x, 1 - y, z, c)]):
        copy = send(box.at[i], box.at[7 + i], (sems.at[0, i], sems.at[1, i]), other)
        copy.start()
        copy.wait()
        box[i + 1] = box[i] + box[7 + i]
    copies = [
        send(box.at[3], box.at[3 + hop], (sems.at[0, 2 + hop], sems.at[1, 2 + hop]), (x, y, (z + hop) % 4, c)) for hop in (1, 2, 3)
    ]
    for copy in copies:
        copy.start()
    for copy in copies:
        copy.wait()
    total[...] = (box[3] + box[5]) + (box[4] + box[6])


def sum_kernel(dg, du, dd, out, total, own, fromtwin, fromfar, fromnear, fromz, squares, box, sems, last, load):
    x, y, z, c = place()
    squares[...] = jnp.zeros_like(squares)
    greet()
    bufs = (own, fromtwin, fromfar, fromnear, fromz, sems, out, squares)

    def tick(t, _):
        @pl.when(t < CHUNKS)
        def _():
            lay, r = 1 - t // 12, t % 12
            color = t % 2

            def fill(go):
                for b in range(4):
                    bx, by = b // 2, b % 2
                    spot = bx * 8 + by * 4 + color * (by * 8 + bx * 4 - bx * 8 - by * 4)
                    for rail in range(2):
                        same = 1 - (rail - c) * (rail - c)
                        s = same * (t % SLOTS) + (1 - same) * (SLOTS + t % 2)
                        for j in range(4):
                            dst = own.at[s, pl.ds(spot, 4), j]
                            q = r // 2

                            @pl.when(jnp.logical_and(r < 8, r % 2 == 0))
                            def _():
                                cp = pltpu.make_async_copy(dg.at[lay, bx, by, :, rail, :, pl.ds(q * 1024 + j * 256, 256)], dst, load.at[b, rail, j])
                                go(cp)

                            @pl.when(jnp.logical_and(r < 8, r % 2 == 1))
                            def _():
                                cp = pltpu.make_async_copy(du.at[lay, bx, by, :, rail, :, pl.ds(q * 1024 + j * 256, 256)], dst, load.at[b, rail, j])
                                go(cp)

                            @pl.when(r >= 8)
                            def _():
                                cp = pltpu.make_async_copy(
                                    dd.at[lay, bx, by, :, rail, pl.ds(32 * j, 32), pl.ds((r - 8) * 256, 256)], dst, load.at[b, rail, j]
                                )
                                go(cp)

            fill(lambda cp: cp.start())
            fill(lambda cp: cp.wait())

        sum_tick(t, bufs)
        return 0

    lax.fori_loop(0, CHUNKS + SUM_AT[-1], tick, 0)
    all_squares(squares, total, box, last)


def summed(dg, du, dd):
    block = (4, 32, 256)
    return pl.pallas_call(
        sum_kernel,
        name="summed",
        out_shape=[jax.ShapeDtypeStruct((CHUNKS,) + block, BF), jax.ShapeDtypeStruct((8, 128), F32)],
        in_specs=[pl.BlockSpec(memory_space=pl.ANY)] * 3,
        out_specs=[pl.BlockSpec(memory_space=pltpu.VMEM)] * 2,
        scratch_shapes=[
            pltpu.VMEM((SLOTS + 2, 16) + block, BF),
            pltpu.VMEM((SLOTS, 16) + block, BF),
            pltpu.VMEM((SLOTS, 8) + block, BF),
            pltpu.VMEM((SLOTS, 4) + block, BF),
            pltpu.VMEM((SLOTS, 3) + block, BF),
            pltpu.VMEM((8, 256), F32),
            pltpu.VMEM((10, 8, 128), F32),
            pltpu.SemaphoreType.DMA((2, SLOTS, 6)),
            pltpu.SemaphoreType.DMA((2, 6)),
            pltpu.SemaphoreType.DMA((4, 2, 4)),
        ],
        compiler_params=pltpu.CompilerParams(collective_id=1, has_side_effects=True, vmem_limit_bytes=48 * 2**20),
    )(dg, du, dd)


def solution(mesh):
    def step(x, dy, *arrays):
        weights, m, v = (arrays[i : i + 3] for i in (0, 3, 6))
        full = [w.reshape(-1, w.shape[-1]) for w in gathered(weights)]
        whole = [dict(zip(NAMES, full[3 * n : 3 * n + 3], strict=True)) for n in range(2)]
        h0, by_h = x[0], dy[0]
        h1 = layer(h0, whole[0])
        grads = [None, None]
        for n, h in ((1, h1), (0, h0)):
            _, back = jax.vjp(lambda w, h: layer(h, w), whole[n], h)
            grads[n], by_h = back(by_h)
        dg, du, dd = (jnp.stack([grads[n][name].reshape(2, 2, 4, 2, -1, grads[n][name].shape[-1]) for n in range(2)]) for name in NAMES)
        sums, squares = summed(dg, du, dd)
        sums = sums.reshape(2, 12, 4, 32, 256)[::-1]
        mine = []
        for i in range(2):
            mine.append(sums[:, i:8:2].transpose(0, 3, 1, 2, 4).reshape(2, 32, 4096))
        mine.append(sums[:, 8:].transpose(0, 2, 3, 1, 4).reshape(2, 128, 1024))
        count = 32 * sum(g.size for g in mine)
        factor = jnp.minimum(1.0, 0.5 * lax.rsqrt(squares[0, 0] / count + 1e-30))
        new = [adamw(w.astype(F32), m, v, g.astype(F32) * factor) for w, m, v, g in zip(weights, m, v, mine, strict=True)]
        return tuple(one[which] for which in range(3) for one in new)

    states, cut = P(("rep", "dp"), None, None), P(None, "dp", None)
    return jax.shard_map(
        step,
        mesh=mesh,
        in_specs=(states, states) + (cut,) * 9,
        out_specs=(P("rep", "dp", None),) * 9,
        check_vma=False,
    )
```

```python
import jax
import jax.numpy as jnp
from jax import lax
from jax.experimental import pallas as pl
from jax.experimental.pallas import tpu as pltpu
from jax.sharding import PartitionSpec as P

BF, F32 = jnp.bfloat16, jnp.float32
MESH = pl.DeviceIdType.MESH
CHUNKS = 24
SLOTS, OWN, OTHER = 6, 7, 3


def adamw(w, m, v, g):
    m = 0.9 * m + 0.1 * g
    v = 0.95 * v + 0.05 * g * g
    step = m * lax.rsqrt(v + 1e-8) + 0.1 * w
    return (w - 0.02 * step).astype(jnp.bfloat16), m, v


def place():
    me = lax.axis_index("dp")
    return me // 16, (me // 8) % 2, (me // 2) % 4, me % 2


def number(x, y, z, c):
    return ((x * 2 + y) * 4 + z) * 2 + c


def greet():
    x, y, z, c = place()
    barrier = pltpu.get_barrier_semaphore()
    others = [(1 - x, y, z, c), (x, 1 - y, z, c), (x, y, z, 1 - c)]
    others += [(x, y, (z + hop) % 4, c) for hop in (1, 2, 3)]
    for other in others:
        pl.semaphore_signal(barrier, 1, device_id={"dp": number(*other)}, device_id_type=MESH)
    pl.semaphore_wait(barrier, len(others))


def send(src, dst, sems, where):
    return pltpu.make_async_remote_copy(
        src_ref=src, dst_ref=dst, send_sem=sems[0], recv_sem=sems[1], device_id={"dp": number(*where)}, device_id_type=MESH
    )


def gather_chunks():
    wide = [[(3 * n + i, 1024 * q, 1024) for q in range(4) for i in (0, 1)] for n in range(2)]
    tall = [[(3 * n + 2, 256 * q, 256) for q in range(4)] for n in range(2)]
    return wide[0] + tall[0] + tall[1] + wide[1]


GATHER_AT = (0, 2, 4, 6, 8)


def gather_tick(t, shards, whole, sems):
    x, y, z, c = place()
    chunks = gather_chunks()

    def copies(k, stage):
        i, first, columns = chunks[k]
        cut = pl.ds(first, columns)
        full = whole[i]

        def pair(n):
            return sems.at[0, k, n], sems.at[1, k, n]

        near = (x, 1 - y, z, c) if k % 2 == 0 else (1 - x, y, z, c)
        far = (1 - x, y, z, c) if k % 2 == 0 else (x, 1 - y, z, c)
        twin = (x, y, z, 1 - c)
        if stage == 0:
            own = full.at[x, y, z, c, :, cut]
            return [lambda hop=hop: send(shards[i].at[:, cut], own, pair(hop - 1), (x, y, (z + hop) % 4, c)) for hop in (1, 2, 3)]
        if stage == 1:
            part = full.at[x, y, :, c, :, cut]
            return [lambda: send(part, part, pair(3), near), lambda: send(part, part, pair(4), twin)]
        if stage == 2:
            part = full.at[x, :, :, c, :, cut] if k % 2 == 0 else full.at[:, y, :, c, :, cut]
            late = full.at[x, 1 - y, :, c, :, cut] if k % 2 == 0 else full.at[1 - x, y, :, c, :, cut]
            return [lambda: send(part, part, pair(5), far), lambda: send(late, late, pair(6), twin)]
        part = full.at[1 - x, :, :, c, :, cut] if k % 2 == 0 else full.at[:, 1 - y, :, c, :, cut]
        return [lambda: send(part, part, pair(7), twin)]

    for stage in (4, 3, 2, 1, 0):
        k = t - GATHER_AT[stage]
        if not 0 <= k < CHUNKS:
            continue
        if stage in (1, 2, 3):
            for copy in copies(k, stage - 1)[: 3 if stage == 1 else 1]:
                copy().wait_recv()
        if stage == 4:
            for copy in copies(k, 1)[1:] + copies(k, 2)[1:] + copies(k, 3):
                copy().wait_recv()
            for past in range(4):
                for copy in copies(k, past):
                    copy().wait_send()
        else:
            for copy in copies(k, stage):
                copy().start()


SUM_AT = (0, 1, 3, 4, 5)


def wide(ref, *at):
    return ref[at].astype(F32)


def sum_stages(k, own, fromtwin, fromfar, fromnear, fromz, sems, out, squares):
    x, y, z, c = place()
    slot, mine, color = k % SLOTS, k % OWN, k % 2
    f, n = x + color * (y - x), y + color * (x - y)
    far = (x + (1 - color) * (1 - 2 * x), y + color * (1 - 2 * y), z, c)
    near = (x + color * (1 - 2 * x), y + (1 - color) * (1 - 2 * y), z, c)

    def pair(i):
        return sems.at[0, slot, i], sems.at[1, slot, i]

    def to_twin():
        return send(own.at[OWN + k % OTHER], fromtwin.at[slot], pair(0), (x, y, z, 1 - c))

    def to_far():
        return send(fromtwin.at[slot, pl.ds((1 - f) * 8, 8)], fromfar.at[slot], pair(1), far)

    def to_near():
        return send(fromtwin.at[slot, pl.ds(f * 8 + (1 - n) * 4, 4)], fromnear.at[slot], pair(2), near)

    base = f * 8 + n * 4

    def to_z(hop):
        to = (z + hop) % 4
        return send(fromtwin.at[slot, base + to], fromz.at[slot, hop - 1], pair(2 + hop), (x, y, to, c))

    def first():
        to_twin().start()

    def second():
        to_twin().wait()

        def add(i, _):
            p = (1 - f) * 8 + i
            fromtwin[slot, p] = (wide(own, mine, p) + wide(fromtwin, slot, p)).astype(BF)
            return 0

        lax.fori_loop(0, 8, add, 0)
        to_far().start()

    def third():
        to_far().wait_recv()

        def add(i, _):
            q = (1 - n) * 4 + i
            p = f * 8 + q
            fromtwin[slot, p] = (wide(own, mine, p) + wide(fromtwin, slot, p) + wide(fromfar, slot, q)).astype(BF)
            return 0

        lax.fori_loop(0, 4, add, 0)
        to_near().start()

    def fourth():
        to_near().wait_recv()
        for hop in (1, 2, 3):
            to = (z + hop) % 4
            p, q = base + to, n * 4 + to
            total = wide(own, mine, p) + wide(fromtwin, slot, p) + wide(fromfar, slot, q) + wide(fromnear, slot, to)
            fromtwin[slot, p] = total.astype(BF)
            to_z(hop).start()

    def fifth():
        for hop in (1, 2, 3):
            to_z(hop).wait()
        to_far().wait_send()
        to_near().wait_send()
        p, q = base + z, n * 4 + z
        total = wide(own, mine, p) + wide(fromtwin, slot, p) + wide(fromfar, slot, q) + wide(fromnear, slot, z)
        total = (total + wide(fromz, slot, 0) + wide(fromz, slot, 1) + wide(fromz, slot, 2)).astype(BF)
        out[k] = total
        square = total.astype(F32)
        square = square * square
        squares[...] += jnp.sum(square.reshape(16, 8, 256), axis=0)

    return first, second, third, fourth, fifth


def sum_tick(t, bufs):
    for stage in (4, 3, 2, 1, 0):
        k = t - SUM_AT[stage]

        @pl.when(jnp.logical_and(k >= 0, k < CHUNKS))
        def _():
            sum_stages(k, *bufs)[stage]()


def all_squares(squares, total, box, sems):
    x, y, z, c = place()
    box[0] = jnp.broadcast_to(jnp.sum(squares[...]), (8, 128))
    for i, other in enumerate([(x, y, z, 1 - c), (1 - x, y, z, c), (x, 1 - y, z, c)]):
        copy = send(box.at[i], box.at[7 + i], (sems.at[0, i], sems.at[1, i]), other)
        copy.start()
        copy.wait()
        box[i + 1] = box[i] + box[7 + i]
    copies = [
        send(box.at[3], box.at[3 + hop], (sems.at[0, 2 + hop], sems.at[1, 2 + hop]), (x, y, (z + hop) % 4, c)) for hop in (1, 2, 3)
    ]
    for copy in copies:
        copy.start()
    for copy in copies:
        copy.wait()
    total[...] = (box[3] + box[5]) + (box[4] + box[6])


NN, NT, TN = (((1,), (0,)), ((), ())), (((1,), (1,)), ((), ())), (((0,), (0,)), ((), ()))


def dot(a, b, dims):
    return lax.dot_general(a, b, dims, preferred_element_type=F32)


def loop(n, body):
    lax.fori_loop(0, n, lambda i, _: (body(i), 0)[1], 0)


def rows(i):
    return pl.ds(pl.multiple_of(i * 1024, 1024), 1024)


def half(i):
    return pl.ds(pl.multiple_of(i * 512, 512), 512)


def keep_wide(own, k, n, r, c):
    color = k % 2
    for b in range(4):
        bx, by = b // 2, b % 2
        spot = bx * 8 + by * 4 + color * (by * 4 - bx * 4)
        for j in range(2):
            part = r[256 * b : 256 * b + 256, 256 * j : 256 * j + 256].astype(BF).reshape(4, 2, 32, 256)
            for rail in range(2):
                same = 1 - (rail - c) * (rail - c)
                at = same * (k % OWN) + (1 - same) * (OWN + k % OTHER)
                own[at, pl.ds(spot, 4), 2 * n + j] = part[:, rail]


def keep_tall(own, k, b, r, c):
    color, bx, by = k % 2, b // 2, b % 2
    spot = bx * 8 + by * 4 + color * (by * 4 - bx * 4)
    part = r.astype(BF).reshape(4, 2, 4, 32, 256)
    for rail in range(2):
        same = 1 - (rail - c) * (rail - c)
        at = same * (k % OWN) + (1 - same) * (OWN + k % OTHER)
        own[at, pl.ds(spot, 4)] = part[:, rail]


def step_kernel(*refs):
    (x_in, dy_in), stacked = refs[0:2], refs[2:5]
    shards = [w.at[n] for n in range(2) for w in stacked]
    out, total, whole = refs[5], refs[6], refs[7:13]
    acts, silus, slopes, douts, h1, a0 = refs[13:19]
    A, B, D, W, F, S, own, fromtwin, fromfar, fromnear, fromz, squares, box = refs[19:32]
    gsems, glocal, ssems, last, load, tiles = refs[32:38]
    x, y, z, c = place()
    bufs = (own, fromtwin, fromfar, fromnear, fromz, ssems, out, squares)
    copy = pltpu.make_async_copy

    def staged(i, j):
        to = whole[i].at[x, y, z, c]
        if i % 3 == 2:
            return shards[i], W.at[1, pl.ds(128 * (i // 3), 128)], to
        cut = pl.ds(1024 * j, 1024)
        return shards[i].at[:, cut], W.at[0, pl.ds(32 * (16 * (i // 3) + 4 * (i % 3) + j), 32)], to.at[:, cut]

    pieces = [(i, j) for i in range(6) for j in range(1 if i % 3 == 2 else 4)]
    for at, (i, j) in enumerate(pieces):
        copy(*staged(i, j)[:2], glocal.at[at]).start()
    copy(x_in, D.at[0], load.at[0]).start()
    copy(dy_in, B, load.at[1]).start()
    squares[...] = jnp.zeros_like(squares)
    greet()

    def tick(t):
        gather_tick(t, shards, whole, gsems)

    def ticks_at(step, table):
        for at, t in table:
            pl.when(step == at)(lambda t=t: tick(t))

    for at, (i, j) in enumerate(pieces):
        copy(*staged(i, j)[:2], glocal.at[at]).wait()
        copy(*staged(i, j)[1:], glocal.at[at]).start()
    tick(0)
    tick(1)
    for at, (i, j) in enumerate(pieces):
        copy(*staged(i, j)[1:], glocal.at[at]).wait()
    tick(2)
    tick(3)
    copy(x_in, D.at[0], load.at[0]).wait()

    def norm(h):
        wide_h = h.astype(F32)
        return (wide_h * lax.rsqrt(jnp.mean(wide_h * wide_h, -1, keepdims=True) + 1e-6)).astype(BF)

    def first_norm(i):
        at = pl.ds(pl.multiple_of(i * 128, 128), 128)
        A[at] = norm(D[0, at])

    loop(16, first_norm)
    copy(A, a0, load.at[0]).start()
    for t in range(4, 10):
        tick(t)
    copy(A, a0, load.at[0]).wait()

    def wide_quarter(i, q, b):
        return copy(whole[i].at[:, :, :, :, :, rows(q)], W.at[b].reshape(2, 2, 4, 2, 32, 1024), load.at[2 + b])

    def tall_quarter(i, q, b):
        return copy(whole[i].at[q // 2, q % 2], W.at[b].reshape(4, 2, 128, 1024), load.at[2 + b])

    def phase_gu0():
        def gate_up_0(q):
            wide_quarter(0, q, 0).start()
            wide_quarter(1, q, 1).start()
            wide_quarter(0, q, 0).wait()
            wide_quarter(1, q, 1).wait()
            b = q % 2

            @pl.when(q >= 2)
            def _():
                copy(D.at[b], acts.at[0, q - 2], load.at[4 + b]).wait()

            def tile(i):
                ticks_at(4 * q + i, [(2 * j, 10 + j) for j in range(8)])
                m, n, e = i // 2, i % 2, i % 2
                number_of = 4 * q + i

                @pl.when(number_of >= 2)
                def _():
                    copy(F.at[e], silus.at[number_of - 2], tiles.at[0, e]).wait()
                    copy(F.at[2 + e], slopes.at[number_of - 2], tiles.at[1, e]).wait()

                gate = dot(A[rows(m)], W[0, :, half(n)], NN)
                up = dot(A[rows(m)], W[1, :, half(n)], NN)
                s = jax.nn.sigmoid(gate)
                silu = gate * s
                F[e] = silu
                F[2 + e] = up * (s + silu * (1 - s))
                D[b, rows(m), half(n)] = (silu * up).astype(BF)
                copy(F.at[e], silus.at[number_of], tiles.at[0, e]).start()
                copy(F.at[2 + e], slopes.at[number_of], tiles.at[1, e]).start()

            loop(4, tile)
            copy(D.at[b], acts.at[0, q], load.at[4 + b]).start()

        loop(4, gate_up_0)
        for e in range(2):
            copy(F.at[e], silus.at[14 + e], tiles.at[0, e]).wait()
            copy(F.at[2 + e], slopes.at[14 + e], tiles.at[1, e]).wait()
            copy(D.at[e], acts.at[0, 2 + e], load.at[4 + e]).wait()

    phase_gu0()
    tick(18)
    tick(19)

    def act_quarter(n, q, b):
        return copy(acts.at[n, q], D.at[b], load.at[4 + b])

    def phase_down0():
        tall_quarter(2, 0, 0).start()
        act_quarter(0, 0, 0).start()

        def down_0(q):
            b = q % 2
            tall_quarter(2, q, b).wait()
            act_quarter(0, q, b).wait()

            @pl.when(q < 3)
            def _():
                tall_quarter(2, q + 1, 1 - b).start()
                act_quarter(0, q + 1, 1 - b).start()

            def tile(i):
                ticks_at(4 * q + i, [(4 * j, 20 + j) for j in range(4)])
                m, n = i // 2, i % 2
                part = dot(D[b, rows(m)], W[b, :, half(n)], NN)

                @pl.when(q == 0)
                def _():
                    F[i] = part

                @pl.when(q > 0)
                def _():
                    F[i] += part

            loop(4, tile)

        loop(4, down_0)

    phase_down0()
    copy(x_in, D.at[0], load.at[0]).start()
    copy(dy_in, B, load.at[1]).wait()
    copy(x_in, D.at[0], load.at[0]).wait()

    def phase_norm2():
        def second_norm(i):
            at = pl.ds(pl.multiple_of(i * 128, 128), 128)
            m, r = i // 8, pl.ds(pl.multiple_of(i % 8 * 128, 128), 128)
            for n in range(2):
                cut = pl.ds(512 * n, 512)
                D[1, at, cut] = (D[0, at, cut].astype(F32) + F[2 * m + n, r].astype(BF).astype(F32)).astype(BF)
            A[at] = norm(D[1, at])

        loop(16, second_norm)

    phase_norm2()
    copy(D.at[1], h1, load.at[0]).start()

    def phase_hid1():
        tall_quarter(5, 0, 0).start()

        def by_hidden_1(q):
            b = q % 2
            tall_quarter(5, q, b).wait()

            @pl.when(q < 3)
            def _():
                tall_quarter(5, q + 1, 1 - b).start()

            def tile(i):
                ticks_at(4 * q + i, [(8 * j, 24 + j) for j in range(2)])
                m, n, e = i // 2, i % 2, i % 2
                number_of = 4 * q + i

                @pl.when(number_of >= 2)
                def _():
                    copy(S.at[e], douts.at[number_of - 2], tiles.at[0, e]).wait()

                S[e] = dot(B[rows(m)], W[b, half(n)], NT).astype(BF)
                copy(S.at[e], douts.at[number_of], tiles.at[0, e]).start()

            loop(4, tile)

        loop(4, by_hidden_1)
        for e in range(2):
            copy(S.at[e], douts.at[14 + e], tiles.at[0, e]).wait()

    phase_hid1()
    copy(D.at[1], h1, load.at[0]).wait()

    def wide_gradient(k, i):
        def part(n):
            keep_wide(own, k, n, dot(A[...], D[i, :, half(n)], TN), c)

        loop(2, part)
        sum_tick(k, bufs)

    def phase_l1():
        wide_quarter(3, 0, 0).start()
        wide_quarter(4, 0, 1).start()

        def layer_1(q):
            wide_quarter(3, q, 0).wait()
            wide_quarter(4, q, 1).wait()
            copy(douts.at[4 * q], S.at[0], tiles.at[0, 0]).start()

            def tile(i):
                ticks_at(4 * q + i, [(j, 26 + j) for j in range(6)])
                m, n, e = i // 2, i % 2, i % 2
                number_of = 4 * q + i
                copy(douts.at[number_of], S.at[e], tiles.at[0, e]).wait()

                @pl.when(i < 3)
                def _():
                    copy(douts.at[number_of + 1], S.at[1 - e], tiles.at[0, 1 - e]).start()

                @pl.when(number_of >= 2)
                def _():
                    copy(S.at[2 + e], acts.at[1, q, rows(m), half(n)], tiles.at[1, e]).wait()

                def part(j):
                    here = pl.ds(pl.multiple_of(j * 512, 512), 512)
                    there = pl.ds(pl.multiple_of(m * 1024 + j * 512, 512), 512)
                    gate = dot(A[there], W[0, :, half(n)], NN)
                    up = dot(A[there], W[1, :, half(n)], NN)
                    by_act = S[e, here].astype(F32)
                    s = jax.nn.sigmoid(gate)
                    silu = gate * s
                    S[2 + e, here] = (silu * up).astype(BF)
                    D[1, there, half(n)] = (by_act * silu).astype(BF)
                    D[0, there, half(n)] = (by_act * (up * (s + silu * (1 - s)))).astype(BF)

                loop(1024 // 512, part)
                copy(S.at[2 + e], acts.at[1, q, rows(m), half(n)], tiles.at[1, e]).start()

            loop(4, tile)

            def back(i):
                m, n = i // 2, i % 2
                part = dot(D[0, rows(m)], W[0, half(n)], NT) + dot(D[1, rows(m)], W[1, half(n)], NT)

                @pl.when(q == 0)
                def _():
                    F[i] = part

                @pl.when(q > 0)
                def _():
                    F[i] += part

            loop(4, back)

            @pl.when(q < 3)
            def _():
                wide_quarter(3, q + 1, 0).start()
                wide_quarter(4, q + 1, 1).start()

            loop(2, lambda i: wide_gradient(2 * q + i, i))

        loop(4, layer_1)
        for e in range(2):
            copy(S.at[2 + e], acts.at[1, 3, rows(1), half(e)], tiles.at[1, e]).wait()


    phase_l1()
    def tall_gradient(n, k):
        act_quarter(n, 0, 0).start()

        def part(i):
            p, q, b = i // 4, i % 4, i % 2
            act_quarter(n, q, b).wait()

            @pl.when(i < 7)
            def _():
                act_quarter(n, (i + 1) % 4, 1 - b).start()

            r = dot(D[b], B[:, half(p)], TN)
            for j in range(2):
                keep_tall(own, k + 2 * p + j, q, r[:, 256 * j : 256 * j + 256], c)

            @pl.when(q == 3)
            def _():
                loop(2, lambda j: sum_tick(k + 2 * p + j, bufs))

        loop(8, part)

    tall_gradient(1, 8)

    copy(h1, D.at[0], load.at[0]).start()
    copy(a0, A, load.at[1]).start()
    copy(h1, D.at[0], load.at[0]).wait()

    def phase_nback():
        def norm_back(i):
            at = pl.ds(pl.multiple_of(i * 128, 128), 128)
            m, r = i // 8, pl.ds(pl.multiple_of(i % 8 * 128, 128), 128)
            h = D[0, at].astype(F32)
            scale = lax.rsqrt(jnp.mean(h * h, -1, keepdims=True) + 1e-6)
            by_a = [F[2 * m + n, r].astype(BF).astype(F32) for n in range(2)]
            parts = [h[:, 512 * n : 512 * n + 512] for n in range(2)]
            along = sum(jnp.sum(one * part, -1, keepdims=True) for one, part in zip(by_a, parts, strict=True))
            along = along * (scale * scale * scale) * (1 / 1024)
            for n in range(2):
                cut = pl.ds(512 * n, 512)
                by_h = (by_a[n] * scale - parts[n] * along).astype(BF)
                B[at, cut] = (B[at, cut].astype(F32) + by_h.astype(F32)).astype(BF)

        loop(16, norm_back)

    phase_nback()
    tall_gradient(0, 12)

    def kept_tile(number_of, e):
        return (
            copy(silus.at[number_of], F.at[e], tiles.at[0, e]),
            copy(slopes.at[number_of], F.at[2 + e], tiles.at[1, e]),
        )

    copy(a0, A, load.at[1]).wait()
    def phase_l0():
        tall_quarter(2, 0, 0).start()
        for one in kept_tile(0, 0):
            one.start()

        def layer_0(q):
            b = q % 2
            tall_quarter(2, q, b).wait()

            @pl.when(q < 3)
            def _():
                tall_quarter(2, q + 1, 1 - b).start()

            def tile(i):
                m, n, e = i // 2, i % 2, i % 2
                number_of = 4 * q + i
                for one in kept_tile(number_of, e):
                    one.wait()

                @pl.when(number_of < 15)
                def _():
                    for one in kept_tile(number_of + 1, 1 - e):
                        one.start()

                by_act = dot(B[rows(m)], W[b, half(n)], NT).astype(BF).astype(F32)
                D[1, rows(m), half(n)] = (by_act * F[e]).astype(BF)
                D[0, rows(m), half(n)] = (by_act * F[2 + e]).astype(BF)

            loop(4, tile)
            loop(2, lambda i: wide_gradient(16 + 2 * q + i, i))

        loop(4, layer_0)

    phase_l0()
    loop(SUM_AT[-1], lambda t: sum_tick(CHUNKS + t, bufs))
    all_squares(squares, total, box, last)


def stepped(x, dy, weights):
    shards = [jax.ShapeDtypeStruct(w.shape[1:], BF) for n in range(2) for w in weights]
    block, hbm = (4, 32, 256), pl.BlockSpec(memory_space=pl.ANY)
    shape = jax.ShapeDtypeStruct
    results = pl.pallas_call(
        step_kernel,
        name="step",
        out_shape=[shape((CHUNKS,) + block, BF), shape((8, 128), F32)]
        + [shape((2, 2, 4, 2) + s.shape, BF) for s in shards]
        + [
            shape((2, 4, 2048, 1024), BF),
            shape((16, 1024, 512), F32),
            shape((16, 1024, 512), F32),
            shape((16, 1024, 512), BF),
            shape((2048, 1024), BF),
            shape((2048, 1024), BF),
        ],
        in_specs=[hbm] * 5,
        out_specs=[pl.BlockSpec(memory_space=pltpu.VMEM)] * 2 + [hbm] * 12,
        scratch_shapes=[
            pltpu.VMEM((2048, 1024), BF),
            pltpu.VMEM((2048, 1024), BF),
            pltpu.VMEM((2, 2048, 1024), BF),
            pltpu.VMEM((2, 1024, 1024), BF),
            pltpu.VMEM((4, 1024, 512), F32),
            pltpu.VMEM((4, 1024, 512), BF),
            pltpu.VMEM((OWN + OTHER, 16) + block, BF),
            pltpu.VMEM((SLOTS, 16) + block, BF),
            pltpu.VMEM((SLOTS, 8) + block, BF),
            pltpu.VMEM((SLOTS, 4) + block, BF),
            pltpu.VMEM((SLOTS, 3) + block, BF),
            pltpu.VMEM((8, 256), F32),
            pltpu.VMEM((10, 8, 128), F32),
            pltpu.SemaphoreType.DMA((2, CHUNKS, 8)),
            pltpu.SemaphoreType.DMA((18,)),
            pltpu.SemaphoreType.DMA((2, SLOTS, 6)),
            pltpu.SemaphoreType.DMA((2, 6)),
            pltpu.SemaphoreType.DMA((6,)),
            pltpu.SemaphoreType.DMA((2, 2)),
        ],
        compiler_params=pltpu.CompilerParams(collective_id=0, has_side_effects=True, vmem_limit_bytes=67043328),
    )(x, dy, *weights)
    return results[0], results[1]


def solution(mesh):
    def step(x, dy, *arrays):
        weights, m, v = (arrays[i : i + 3] for i in (0, 3, 6))
        sums, squares = stepped(x[0], dy[0], weights)
        layers = [
            [sums[0:8:2], sums[1:8:2], sums[8:12]],
            [sums[16::2], sums[17::2], sums[12:16]],
        ]
        mine = [jnp.stack([layers[1 - n][i].transpose(2, 0, 1, 3).reshape(32, 4096) for n in range(2)]) for i in range(2)]
        mine.append(jnp.stack([layers[1 - n][2].transpose(1, 2, 0, 3).reshape(128, 1024) for n in range(2)]))
        count = 32 * sum(g.size for g in mine)
        factor = jnp.minimum(1.0, 0.5 * lax.rsqrt(squares[0, 0] / count + 1e-30))
        new = [adamw(w.astype(F32), m, v, g.astype(F32) * factor) for w, m, v, g in zip(weights, m, v, mine, strict=True)]
        return tuple(one[which] for which in range(3) for one in new)

    states, cut = P(("rep", "dp"), None, None), P(None, "dp", None)
    return jax.shard_map(
        step,
        mesh=mesh,
        in_specs=(states, states) + (cut,) * 9,
        out_specs=(P("rep", "dp", None),) * 9,
        check_vma=False,
    )
```

```python
import jax
import jax.numpy as jnp
from jax import lax
from jax.experimental import pallas as pl
from jax.experimental.pallas import tpu as pltpu
from jax.sharding import PartitionSpec as P

BF, F32 = jnp.bfloat16, jnp.float32
MESH = pl.DeviceIdType.MESH
CHUNKS = 48
SLOTS, OWN, OTHER = 12, 15, 8


def adamw(w, m, v, g):
    m = 0.9 * m + 0.1 * g
    v = 0.95 * v + 0.05 * g * g
    step = m * lax.rsqrt(v + 1e-8) + 0.1 * w
    return (w - 0.02 * step).astype(jnp.bfloat16), m, v


HERE = []


def find():
    me = lax.axis_index("dp")
    HERE[:] = [lax.div(me, 16), lax.rem(lax.div(me, 8), 2), lax.rem(lax.div(me, 2), 4), lax.rem(me, 2)]


def place():
    return tuple(HERE)


def mod(a, b):
    return a % b if isinstance(a, int) else lax.rem(a, b)


def div(a, b):
    return a // b if isinstance(a, int) else lax.div(a, b)


def number(x, y, z, c):
    return ((x * 2 + y) * 4 + z) * 2 + c


def greet():
    x, y, z, c = place()
    barrier = pltpu.get_barrier_semaphore()
    others = [(1 - x, y, z, c), (x, 1 - y, z, c), (x, y, z, 1 - c)]
    others += [(x, y, (z + hop) % 4, c) for hop in (1, 2, 3)]
    for other in others:
        pl.semaphore_signal(barrier, 1, device_id={"dp": number(*other)}, device_id_type=MESH)
    pl.semaphore_wait(barrier, len(others))


def send(src, dst, sems, where):
    return pltpu.make_async_remote_copy(
        src_ref=src, dst_ref=dst, send_sem=sems[0], recv_sem=sems[1], device_id={"dp": number(*where)}, device_id_type=MESH
    )


GATHER_AT = (0, 3, 5, 8, 10)
DONE = GATHER_AT[-1]


def route(k):
    x, y, z, c = place()
    color = mod(k, 2)
    f, n = x + color * (y - x), y + color * (x - y)
    far = (x + (1 - color) * (1 - 2 * x), y + color * (1 - 2 * y), z, c)
    near = (x + color * (1 - 2 * x), y + (1 - color) * (1 - 2 * y), z, c)
    ups = [(x, y, (z + hop) & 3, c) for hop in (1, 2, 3)]
    return f, n, z, c, far, near, ups, (x, y, z, 1 - c)


def landed(pieces, pack, sem):
    part = pack.at[pl.ds(0, pieces)]
    pltpu.make_async_copy(part, part, sem).wait()


def gather_copies(k, stage, pack, whole, sent, came):
    f, n, z, c, far, near, ups, twin = route(k)
    every, z_first = slice(None), k % 3 < 2

    def go(i, where, *at):
        part = whole.at[(k,) + at]
        return send(part, part, (sent.at[0], came.at[k, i]), where)

    def own(i, where):
        return send(pack.at[k], whole.at[k, f, n, z, c], (sent.at[1], came.at[k, i]), where)

    if stage == 0:
        return [own(0, up) for up in ups] if z_first else [own(1, near)]
    if stage == 1:
        return [go(1, near, f, n, every, c)] if z_first else [go(0, up, f, every, z, c) for up in ups]
    if stage == 2:
        return [go(2, far, f, every, every, c)]
    return [go(3, twin, every, every, every, c)]


def gather_tick(t, bufs):
    pack, came = bufs[0], bufs[3]
    for stage in (4, 3, 2, 1, 0):
        k = t - GATHER_AT[stage]
        if not 0 <= k < CHUNKS:
            continue
        z_first = k % 3 < 2
        if stage == 1:
            landed(3 if z_first else 1, pack, came.at[k, 0 if z_first else 1])
        if stage == 2:
            landed(4 if z_first else 6, pack, came.at[k, 1 if z_first else 0])
        if stage == 3:
            landed(8, pack, came.at[k, 2])
        if stage == 4:
            landed(16, pack, came.at[k, 3])
        else:
            for copy in gather_copies(k, stage, *bufs):
                copy.start()


SUM_AT = (0, 1, 3, 6, 8)


def wide(ref, *at):
    return ref[at].astype(F32)


def sum_stages(k, own, fromtwin, fromfar, fromnear, fromz, sems, out, squares, put):
    f, n, z, c, far, near, ups, twin = route(k)
    slot, mine = mod(k, SLOTS), mod(k, OWN)
    every = slice(None)

    def pair(i):
        return sems.at[slot, 5], sems.at[slot, 1 + i]

    def two(*at):
        return wide(own, mine, *at) + wide(fromtwin, slot, *at)

    def to_twin():
        return send(own.at[OWN + mod(k, OTHER)], fromtwin.at[slot], (sems.at[slot, 0], sems.at[slot, 1]), twin)

    def to_far():
        return send(fromtwin.at[slot, 1 - f], fromfar.at[slot], pair(1), far)

    def first():
        to_twin().start()

    def second():
        to_twin().wait()

        def add(i, _):
            at = (1 - f, i // 2, pl.ds(2 * (i % 2), 2))
            fromtwin[(slot,) + at] = two(*at).astype(BF)
            return 0

        lax.fori_loop(0, 4, add, 0)
        to_far().start()

    def near_first():
        return send(fromtwin.at[slot, f, 1 - n], fromnear.at[slot], pair(2), near)

    def z_last(hop):
        to = ups[hop][2]
        return send(fromtwin.at[slot, f, n, to], fromz.at[slot, hop, 0], pair(3), ups[hop])

    def third_near():
        to_far().wait_recv()

        def add(i, _):
            at = (1 - n, pl.ds(2 * i, 2))
            fromtwin[(slot, f) + at] = (two(f, *at) + wide(fromfar, slot, *at)).astype(BF)
            return 0

        lax.fori_loop(0, 2, add, 0)
        near_first().start()

    def fourth_near():
        near_first().wait_recv()
        for hop in range(3):
            to = ups[hop][2]
            total = two(f, n, to) + wide(fromfar, slot, n, to) + wide(fromnear, slot, to)
            fromtwin[slot, f, n, to] = total.astype(BF)
            z_last(hop).start()

    def fifth_near():
        landed(3, out, sems.at[slot, 4])
        return wide(fromnear, slot, z) + wide(fromz, slot, 0, 0) + wide(fromz, slot, 1, 0) + wide(fromz, slot, 2, 0)

    def z_first(hop):
        to = ups[hop][2]
        return send(fromtwin.at[slot, f, every, to], fromz.at[slot, hop], pair(3), ups[hop])

    def near_last():
        return send(fromtwin.at[slot, f, 1 - n, z], fromnear.at[slot, 0], pair(2), near)

    def third_z():
        to_far().wait_recv()
        for hop in range(3):
            to = ups[hop][2]
            for i in range(2):
                fromtwin[slot, f, i, to] = (two(f, i, to) + wide(fromfar, slot, i, to)).astype(BF)
            z_first(hop).start()

    def along_z(i):
        return wide(fromz, slot, 0, i) + wide(fromz, slot, 1, i) + wide(fromz, slot, 2, i)

    def fourth_z():
        landed(6, out, sems.at[slot, 4])
        total = two(f, 1 - n, z) + wide(fromfar, slot, 1 - n, z) + along_z(1 - n)
        fromtwin[slot, f, 1 - n, z] = total.astype(BF)
        near_last().start()

    def fifth_z():
        near_last().wait_recv()
        return along_z(n) + wide(fromnear, slot, 0)

    def fifth(rest):
        landed(15, out, sems.at[slot, 5])
        total = (two(f, n, z) + wide(fromfar, slot, n, z) + rest()).astype(BF)
        out[k] = total
        put(k)
        square = total.astype(F32)
        square = square * square
        squares[...] += jnp.sum(square.reshape(16, 8, 128), axis=0)

    def last_near():
        fifth(fifth_near)

    def last_z():
        fifth(fifth_z)

    return (first, second, (third_near, third_z), (fourth_near, fourth_z), (last_near, last_z))


def sum_tick(t, bufs):
    for stage in (4, 3, 2, 1, 0):
        k = t - SUM_AT[stage]

        @pl.when(jnp.logical_and(k >= 0, k < CHUNKS))
        def _():
            if stage < 2:
                sum_stages(k, *bufs)[stage]()
            else:
                pl.when(mod(k, 3) < 2)(lambda: sum_stages(k, *bufs)[stage][0]())
                pl.when(mod(k, 3) >= 2)(lambda: sum_stages(k, *bufs)[stage][1]())


def all_squares(squares, total, box, sems):
    x, y, z, c = place()
    box[0] = jnp.broadcast_to(jnp.sum(squares[...]), (8, 128))
    for i, other in enumerate([(x, y, z, 1 - c), (1 - x, y, z, c), (x, 1 - y, z, c)]):
        copy = send(box.at[i], box.at[7 + i], (sems.at[0, i], sems.at[1, i]), other)
        copy.start()
        copy.wait()
        box[i + 1] = box[i] + box[7 + i]
    copies = [
        send(box.at[3], box.at[3 + hop], (sems.at[0, 2 + hop], sems.at[1, 2 + hop]), (x, y, (z + hop) % 4, c)) for hop in (1, 2, 3)
    ]
    for copy in copies:
        copy.start()
    for copy in copies:
        copy.wait()
    total[...] = (box[3] + box[5]) + (box[4] + box[6])


NN, NT, TN = (((1,), (0,)), ((), ())), (((1,), (1,)), ((), ())), (((0,), (0,)), ((), ()))


def dot(a, b, dims):
    return lax.dot_general(a, b, dims, preferred_element_type=F32)


def loop(n, body):
    lax.fori_loop(0, n, lambda i, _: (body(i), 0)[1], 0)


def rows(i):
    return pl.ds(pl.multiple_of(i * 1024, 1024), 1024)


def half(i):
    return pl.ds(pl.multiple_of(i * 512, 512), 512)


def spots(k, rail, c, b):
    same = 1 - (rail - c) * (rail - c)
    at = same * mod(k, OWN) + (1 - same) * (OWN + mod(k, OTHER))
    color, bx, by = mod(k, 2), div(b, 2), mod(b, 2)
    return at, bx + color * (by - bx), by + color * (bx - by)


def keep_wide(own, k, r, c):
    for b in range(4):
        for j in range(4):
            part = r[256 * b : 256 * b + 256, 128 * j : 128 * j + 128].astype(BF).reshape(4, 2, 32, 128)
            for rail in range(2):
                at, far, near = spots(k, rail, c, b)
                own[at, far, near, :, j] = part[:, rail]


def keep_tall(own, k, b, r, c):
    part = r.astype(BF).reshape(4, 2, 4, 32, 128)
    for rail in range(2):
        at, far, near = spots(k, rail, c, b)
        own[at, far, near] = part[:, rail]


def step_kernel(*refs):
    (x_in, dy_in), shards = refs[0:2], refs[2:5]
    total, grads, whole = refs[5], refs[6:9], refs[9]
    acts, silus, slopes, douts, hidden, h1, a0 = refs[10:17]
    A, B, D, W, F, S, pack, own, fromtwin, fromfar, fromnear, fromz, squares, box = refs[17:31]
    gsems, glocal, ssems, last, load, tiles = refs[31:37]
    find()
    x, y, z, c = place()
    copy = pltpu.make_async_copy

    def packed(k):
        if 16 <= k < 32:
            return [copy(shards[2].at[k // 24].reshape(4, 32, 1024).at[:, :, pl.ds(k % 8 * 128, 128)], pack.at[k], glocal.at[0])]
        first = (k % 32) // 4 * 1024 + (k % 4) // 2 * 512
        return [copy(shards[k % 2].at[k // 32, :, pl.ds(first + 128 * j, 128)], pack.at[k, j], glocal.at[0]) for j in range(4)]

    for k in range(CHUNKS):
        for one in packed(k):
            one.start()
    copy(x_in, D.at[0], load.at[0]).start()
    copy(dy_in, B, load.at[1]).start()
    squares[...] = jnp.zeros_like(squares)
    greet()
    copy(pack, pack, glocal.at[0]).wait()

    def sent_all(i):
        first = sum(3 if k % 3 < 2 else 1 for k in range(CHUNKS))
        part = whole.reshape(32 * CHUNKS, 4, 32, 128).at[pl.ds(0, first if i else 31 * CHUNKS - first)]
        copy(part, part, glocal.at[2 + i]).wait()

    def put(k):
        n, first = 1 - div(k, 24), div(mod(k, 32), 4) * 1024 + mod(k, 2) * 512
        flat = jnp.logical_or(k < 16, k >= 32)
        for i in range(2):

            @pl.when(jnp.logical_and(flat, div(mod(k, 4), 2) == i))
            def _():
                for j in range(4):
                    cut = pl.ds(pl.multiple_of(first + 128 * j, 128), 128)
                    copy(pack.at[k, j], grads[i].at[n, :, cut], glocal.at[0]).start()

        @pl.when(jnp.logical_not(flat))
        def _():
            cut = pl.ds(pl.multiple_of(mod(k, 8) * 128, 128), 128)
            copy(pack.at[k], grads[2].at[n].reshape(4, 32, 1024).at[:, :, cut], glocal.at[0]).start()

    bufs = (own, fromtwin, fromfar, fromnear, fromz, ssems, pack, squares, put)

    def tick(t):
        gather_tick(t, (pack, whole, glocal.at[pl.ds(2, 2)], gsems))

    def ticks_at(step, first, count, every=1):
        for i in range(count):
            pl.when(step == i * every)(lambda i=i: tick(first + i))

    def sum_at(when, t):
        pl.when(when)(lambda: sum_tick(t, bufs))

    tick(0)
    tick(1)
    for k in range(CHUNKS):
        f, n = route(k)[:2]
        copy(pack.at[k], whole.at[k, f, n, z, c], glocal.at[1]).start()
    copy(pack, pack, glocal.at[1]).wait()
    tick(2)
    tick(3)
    copy(x_in, D.at[0], load.at[0]).wait()

    def norm(h):
        wide_h = h.astype(F32)
        return (wide_h * lax.rsqrt(jnp.mean(wide_h * wide_h, -1, keepdims=True) + 1e-6)).astype(BF)

    def first_norm(i):
        at = pl.ds(pl.multiple_of(i * 128, 128), 128)
        A[at] = norm(D[0, at])

    loop(16, first_norm)
    copy(A, a0, load.at[0]).start()
    for t in range(DONE):
        tick(4 + t)
    copy(A, a0, load.at[0]).wait()

    def wide_quarter(n, i, q, b):
        def part(at):
            blk, k = at // 2, 32 * n + 4 * q + 2 * (at % 2) + i
            bx, by = blk // 2, blk % 2
            for j in range(4):
                cut = pl.ds(pl.multiple_of(at % 2 * 512 + 128 * j, 128), 128)
                src = whole.at[k, bx + i * (by - bx), by + i * (bx - by), :, :, j]
                copy(src, W.at[b].reshape(4, 4, 2, 32, 1024).at[blk, :, :, :, cut], load.at[2 + b]).start()

        loop(8, part)

    def tall_quarter(n, q, b):
        def part(j):
            color, bx, by = j % 2, q // 2, q % 2
            cut = pl.ds(pl.multiple_of(128 * j, 128), 128)
            src = whole.at[16 + 8 * n + j, bx + color * (by - bx), by + color * (bx - by)]
            copy(src, W.at[b].reshape(4, 2, 4, 32, 1024).at[:, :, :, :, cut], load.at[2 + b]).start()

        loop(8, part)

    def loaded(b):
        copy(W.at[b], W.at[b], load.at[2 + b]).wait()

    def phase_gu0():
        def gate_up_0(q):
            wide_quarter(0, 0, q, 0)
            wide_quarter(0, 1, q, 1)
            loaded(0)
            loaded(1)
            b = q % 2

            @pl.when(q >= 2)
            def _():
                copy(D.at[b], acts.at[0, q - 2], load.at[4 + b]).wait()

            def tile(i):
                ticks_at(4 * q + i, DONE + 4, 16)
                m, n, e = i // 2, i % 2, i % 2
                number_of = 4 * q + i

                @pl.when(number_of >= 2)
                def _():
                    copy(F.at[e], silus.at[number_of - 2], tiles.at[0, e]).wait()
                    copy(F.at[2 + e], slopes.at[number_of - 2], tiles.at[1, e]).wait()

                def part(j):
                    here = half(j)
                    there = pl.ds(pl.multiple_of(m * 1024 + j * 512, 512), 512)
                    gate = dot(A[there], W[0, :, half(n)], NN)
                    up = dot(A[there], W[1, :, half(n)], NN)
                    s = jax.nn.sigmoid(gate)
                    silu = gate * s
                    F[e, here] = silu
                    F[2 + e, here] = up * (s + silu * (1 - s))
                    D[b, there, half(n)] = (silu * up).astype(BF)

                loop(2, part)
                copy(F.at[e], silus.at[number_of], tiles.at[0, e]).start()
                copy(F.at[2 + e], slopes.at[number_of], tiles.at[1, e]).start()

            loop(4, tile)
            copy(D.at[b], acts.at[0, q], load.at[4 + b]).start()

        loop(4, gate_up_0)
        for e in range(2):
            copy(F.at[e], silus.at[14 + e], tiles.at[0, e]).wait()
            copy(F.at[2 + e], slopes.at[14 + e], tiles.at[1, e]).wait()
            copy(D.at[e], acts.at[0, 2 + e], load.at[4 + e]).wait()

    phase_gu0()
    for t in range(4):
        tick(DONE + 20 + t)

    def act_quarter(n, q, b):
        return copy(acts.at[n, q], D.at[b], load.at[4 + b])

    def phase_down0():
        tall_quarter(0, 0, 0)
        act_quarter(0, 0, 0).start()

        def down_0(q):
            b = q % 2
            loaded(b)
            act_quarter(0, q, b).wait()

            @pl.when(q < 3)
            def _():
                tall_quarter(0, q + 1, 1 - b)
                act_quarter(0, q + 1, 1 - b).start()

            def tile(i):
                ticks_at(4 * q + i, DONE + 24, 8, 2)
                m, n = i // 2, i % 2
                part = dot(D[b, rows(m)], W[b, :, half(n)], NN)

                @pl.when(q == 0)
                def _():
                    F[i] = part

                @pl.when(q > 0)
                def _():
                    F[i] += part

            loop(4, tile)

        loop(4, down_0)

    phase_down0()
    copy(x_in, D.at[0], load.at[0]).start()
    copy(dy_in, B, load.at[1]).wait()
    copy(x_in, D.at[0], load.at[0]).wait()

    def phase_norm2():
        def second_norm(i):
            at = pl.ds(pl.multiple_of(i * 128, 128), 128)
            m, r = i // 8, pl.ds(pl.multiple_of(i % 8 * 128, 128), 128)
            for n in range(2):
                cut = pl.ds(512 * n, 512)
                D[1, at, cut] = (D[0, at, cut].astype(F32) + F[2 * m + n, r].astype(BF).astype(F32)).astype(BF)
            A[at] = norm(D[1, at])

        loop(16, second_norm)

    phase_norm2()
    copy(D.at[1], h1, load.at[0]).start()

    def phase_hid1():
        tall_quarter(1, 0, 0)

        def by_hidden_1(q):
            b = q % 2
            loaded(b)

            @pl.when(q < 3)
            def _():
                tall_quarter(1, q + 1, 1 - b)

            def tile(i):
                ticks_at(4 * q + i, DONE + 32, 4, 4)
                m, n, e = i // 2, i % 2, i % 2
                number_of = 4 * q + i

                @pl.when(number_of >= 2)
                def _():
                    copy(S.at[e], douts.at[number_of - 2], tiles.at[0, e]).wait()

                S[e] = dot(B[rows(m)], W[b, half(n)], NT).astype(BF)
                copy(S.at[e], douts.at[number_of], tiles.at[0, e]).start()

            loop(4, tile)

        loop(4, by_hidden_1)
        for e in range(2):
            copy(S.at[e], douts.at[14 + e], tiles.at[0, e]).wait()

    phase_hid1()
    copy(D.at[1], h1, load.at[0]).wait()

    def wide_gradient(k, i):
        keep_wide(own, k + i, dot(A[...], D[i // 2, :, half(i % 2)], TN), c)

    def phase_l1():
        wide_quarter(1, 0, 0, 0)
        wide_quarter(1, 1, 0, 1)

        def layer_1(q):
            loaded(0)
            loaded(1)
            pl.when(q == 1)(lambda: sent_all(1))
            copy(douts.at[4 * q], S.at[0], tiles.at[0, 0]).start()

            def tile(i):
                for j in range(6):
                    pl.when(4 * q + i == 4 * (j // 2) + 2 * (j % 2) + 1)(lambda j=j: tick(DONE + 36 + 4 * (j // 2) + j % 2))
                sum_at(i % 2 == 1, 4 * q + i // 2 - 3)
                m, n, e = i // 2, i % 2, i % 2
                number_of = 4 * q + i
                copy(douts.at[number_of], S.at[e], tiles.at[0, e]).wait()

                @pl.when(i < 3)
                def _():
                    copy(douts.at[number_of + 1], S.at[1 - e], tiles.at[0, 1 - e]).start()

                @pl.when(number_of >= 2)
                def _():
                    copy(S.at[2 + e], acts.at[1, q, rows(m), half(n)], tiles.at[1, e]).wait()

                def part(j):
                    here = pl.ds(pl.multiple_of(j * 512, 512), 512)
                    there = pl.ds(pl.multiple_of(m * 1024 + j * 512, 512), 512)
                    gate = dot(A[there], W[0, :, half(n)], NN)
                    up = dot(A[there], W[1, :, half(n)], NN)
                    by_act = S[e, here].astype(F32)
                    s = jax.nn.sigmoid(gate)
                    silu = gate * s
                    S[2 + e, here] = (silu * up).astype(BF)
                    D[1, there, half(n)] = (by_act * silu).astype(BF)
                    D[0, there, half(n)] = (by_act * (up * (s + silu * (1 - s)))).astype(BF)

                loop(1024 // 512, part)
                copy(S.at[2 + e], acts.at[1, q, rows(m), half(n)], tiles.at[1, e]).start()

            loop(4, tile)

            for i in range(2):
                copy(D.at[i], hidden.at[2 * q + i], load.at[4 + i]).start()

            def part(i):
                for j in range(6):
                    pl.when(4 * q + i == 4 * (j // 2) + 2 * (j % 2))(lambda j=j: tick(DONE + 38 + 4 * (j // 2) + j % 2))

                @pl.when(jnp.logical_and(q < 3, i == 3))
                def _():
                    wide_quarter(1, 0, q + 1, 0)
                    wide_quarter(1, 1, q + 1, 1)

                wide_gradient(4 * q, i)
                sum_at(i % 2 == 1, 4 * q + i // 2 - 1)

            loop(4, part)
            for i in range(2):
                copy(D.at[i], hidden.at[2 * q + i], load.at[4 + i]).wait()

        loop(4, layer_1)
        for e in range(2):
            copy(S.at[2 + e], acts.at[1, 3, rows(1), half(e)], tiles.at[1, e]).wait()


    phase_l1()
    sent_all(0)
    def tall_part(b, k, i):
        p, q = i // 4, i % 4
        r = dot(D[b], B[:, half(p)], TN)
        for j in range(4):
            keep_tall(own, k + 4 * p + j, q, r[:, 128 * j : 128 * j + 128], c)

    def back_part(i):
        return copy(hidden.at[i], D.at[0], load.at[4])

    def phase_back():
        def start(i):
            back_part(i).start()

            @pl.when(i % 2 == 0)
            def _():
                wide_quarter(1, 0, i // 2, 0)

            @pl.when(i % 2 == 1)
            def _():
                wide_quarter(1, 1, i // 2, 1)

        start(0)
        act_quarter(1, 0, 1).start()

        def back(i):
            back_part(i).wait()
            loaded(i % 2)

            def tile(j):
                m, n = j // 2, j % 2
                part = dot(D[0, rows(m)], W[i % 2, half(n)], NT)

                @pl.when(i == 0)
                def _():
                    F[j] = part

                @pl.when(i > 0)
                def _():
                    F[j] += part

            loop(4, tile)
            pl.when(i < 7)(lambda: start(i + 1))
            act_quarter(1, i % 4, 1).wait()
            tall_part(1, 16, i)
            pl.when(i < 7)(lambda: act_quarter(1, (i + 1) % 4, 1).start())
            sum_tick(13 + i, bufs)

        loop(8, back)

    phase_back()

    copy(h1, D.at[0], load.at[0]).start()
    copy(a0, A, load.at[1]).start()
    copy(h1, D.at[0], load.at[0]).wait()

    def phase_nback():
        def norm_back(i):
            at = pl.ds(pl.multiple_of(i * 128, 128), 128)
            m, r = i // 8, pl.ds(pl.multiple_of(i % 8 * 128, 128), 128)
            h = D[0, at].astype(F32)
            scale = lax.rsqrt(jnp.mean(h * h, -1, keepdims=True) + 1e-6)
            by_a = [F[2 * m + n, r].astype(BF).astype(F32) for n in range(2)]
            parts = [h[:, 512 * n : 512 * n + 512] for n in range(2)]
            along = sum(jnp.sum(one * part, -1, keepdims=True) for one, part in zip(by_a, parts, strict=True))
            along = along * (scale * scale * scale) * (1 / 1024)
            for n in range(2):
                cut = pl.ds(512 * n, 512)
                by_h = (by_a[n] * scale - parts[n] * along).astype(BF)
                B[at, cut] = (B[at, cut].astype(F32) + by_h.astype(F32)).astype(BF)

        loop(16, norm_back)

    sum_tick(21, bufs)
    phase_nback()
    sum_tick(22, bufs)
    def phase_tall0():
        act_quarter(0, 0, 0).start()

        def part(i):
            b = i % 2
            act_quarter(0, i % 4, b).wait()
            pl.when(i < 7)(lambda: act_quarter(0, (i + 1) % 4, 1 - b).start())
            tall_part(b, 24, i)
            sum_at(i % 2 == 1, 23 + i // 2)

        loop(8, part)

    phase_tall0()

    def kept_tile(number_of, e):
        return (
            copy(silus.at[number_of], F.at[e], tiles.at[0, e]),
            copy(slopes.at[number_of], F.at[2 + e], tiles.at[1, e]),
        )

    copy(a0, A, load.at[1]).wait()
    def phase_l0():
        tall_quarter(0, 0, 0)
        for one in kept_tile(0, 0):
            one.start()

        def layer_0(q):
            b = q % 2
            loaded(b)

            @pl.when(q < 3)
            def _():
                tall_quarter(0, q + 1, 1 - b)

            def tile(i):
                sum_at(i % 2 == 1, 27 + 5 * q + i // 2)
                m, n, e = i // 2, i % 2, i % 2
                number_of = 4 * q + i
                for one in kept_tile(number_of, e):
                    one.wait()

                @pl.when(number_of < 15)
                def _():
                    for one in kept_tile(number_of + 1, 1 - e):
                        one.start()

                by_act = dot(B[rows(m)], W[b, half(n)], NT).astype(BF).astype(F32)
                D[1, rows(m), half(n)] = (by_act * F[e]).astype(BF)
                D[0, rows(m), half(n)] = (by_act * F[2 + e]).astype(BF)

            loop(4, tile)
            def part(i):
                wide_gradient(32 + 4 * q, i)
                sum_at(i != 1, 29 + 5 * q + (i + 1) // 2)

            loop(4, part)

        loop(4, layer_0)

    phase_l0()
    loop(SUM_AT[-1] + 1, lambda t: sum_tick(CHUNKS - 1 + t, bufs))
    all_squares(squares, total, box, last)
    copy(pack, pack, glocal.at[0]).wait()


def stepped(x, dy, weights):
    block, hbm, shape = (4, 32, 128), pl.BlockSpec(memory_space=pl.ANY), jax.ShapeDtypeStruct
    results = pl.pallas_call(
        step_kernel,
        name="step",
        out_shape=[shape((8, 128), F32)]
        + [shape(w.shape, BF) for w in weights]
        + [
            shape((CHUNKS, 2, 2, 4, 2) + block, BF),
            shape((2, 4, 2048, 1024), BF),
            shape((16, 1024, 512), F32),
            shape((16, 1024, 512), F32),
            shape((16, 1024, 512), BF),
            shape((8, 2048, 1024), BF),
            shape((2048, 1024), BF),
            shape((2048, 1024), BF),
        ],
        in_specs=[hbm] * 5,
        out_specs=[pl.BlockSpec(memory_space=pltpu.VMEM)] + [hbm] * 11,
        scratch_shapes=[
            pltpu.VMEM((2048, 1024), BF),
            pltpu.VMEM((2048, 1024), BF),
            pltpu.VMEM((2, 2048, 1024), BF),
            pltpu.VMEM((2, 1024, 1024), BF),
            pltpu.VMEM((4, 1024, 512), F32),
            pltpu.VMEM((4, 1024, 512), BF),
            pltpu.VMEM((CHUNKS,) + block, BF),
            pltpu.VMEM((OWN + OTHER, 2, 2, 4) + block, BF),
            pltpu.VMEM((SLOTS, 2, 2, 4) + block, BF),
            pltpu.VMEM((SLOTS, 2, 4) + block, BF),
            pltpu.VMEM((SLOTS, 4) + block, BF),
            pltpu.VMEM((SLOTS, 3, 2) + block, BF),
            pltpu.VMEM((8, 128), F32),
            pltpu.VMEM((10, 8, 128), F32),
            pltpu.SemaphoreType.DMA((CHUNKS, 4)),
            pltpu.SemaphoreType.DMA((4,)),
            pltpu.SemaphoreType.DMA((SLOTS, 6)),
            pltpu.SemaphoreType.DMA((2, 6)),
            pltpu.SemaphoreType.DMA((6,)),
            pltpu.SemaphoreType.DMA((2, 2)),
        ],
        compiler_params=pltpu.CompilerParams(collective_id=0, has_side_effects=True, vmem_limit_bytes=67043328),
    )(x, dy, *weights)
    return results[0], results[1:4]


def solution(mesh):
    def step(x, dy, *arrays):
        weights, m, v = (arrays[i : i + 3] for i in (0, 3, 6))
        squares, mine = stepped(x[0], dy[0], weights)
        count = 32 * sum(g.size for g in mine)
        factor = jnp.minimum(1.0, 0.5 * lax.rsqrt(squares[0, 0] / count + 1e-30))
        new = [adamw(w.astype(F32), m, v, g.astype(F32) * factor) for w, m, v, g in zip(weights, m, v, mine, strict=True)]
        return tuple(one[which] for which in range(3) for one in new)

    states, cut = P(("rep", "dp"), None, None), P(None, "dp", None)
    return jax.shard_map(
        step,
        mesh=mesh,
        in_specs=(states, states) + (cut,) * 9,
        out_specs=(P("rep", "dp", None),) * 9,
        check_vma=False,
    )
```

```python
import jax
import jax.numpy as jnp
from jax import lax
from jax.experimental import pallas as pl
from jax.experimental.pallas import tpu as pltpu
from jax.sharding import PartitionSpec as P

BF, F32 = jnp.bfloat16, jnp.float32
MESH = pl.DeviceIdType.MESH
CHUNKS = 48
SLOTS, OWN, OTHER, FROMZ = 12, 17, 9, 9


def adamw(w, m, v, g):
    m = 0.9 * m + 0.1 * g
    v = 0.95 * v + 0.05 * g * g
    step = m * lax.rsqrt(v + 1e-8) + 0.1 * w
    return (w - 0.02 * step).astype(jnp.bfloat16), m, v


HERE = []


def find():
    me = lax.axis_index("dp")
    HERE[:] = [lax.div(me, 16), lax.rem(lax.div(me, 8), 2), lax.rem(lax.div(me, 2), 4), lax.rem(me, 2)]


def place():
    return tuple(HERE)


def mod(a, b):
    return a % b if isinstance(a, int) else lax.rem(a, b)


def div(a, b):
    return a // b if isinstance(a, int) else lax.div(a, b)


def number(x, y, z, c):
    return ((x * 2 + y) * 4 + z) * 2 + c


def greet():
    x, y, z, c = place()
    barrier = pltpu.get_barrier_semaphore()
    others = corners()
    others += [(x, y, (z + hop) % 4, c) for hop in (1, 2, 3)]
    for other in others:
        pl.semaphore_signal(barrier, 1, device_id={"dp": number(*other)}, device_id_type=MESH)
    pl.semaphore_wait(barrier, len(others))


def send(src, dst, sems, where):
    return pltpu.make_async_remote_copy(
        src_ref=src, dst_ref=dst, send_sem=sems[0], recv_sem=sems[1], device_id={"dp": number(*where)}, device_id_type=MESH
    )


GATHER_AT = (0, 3, 5, 7, 8)
DONE = GATHER_AT[-1]


def route(k):
    x, y, z, c = place()
    color = mod(k, 2)
    f, n = x + color * (y - x), y + color * (x - y)
    far = (x + (1 - color) * (1 - 2 * x), y + color * (1 - 2 * y), z, c)
    near = (x + color * (1 - 2 * x), y + (1 - color) * (1 - 2 * y), z, c)
    ups = [(x, y, (z + hop) & 3, c) for hop in (1, 2, 3)]
    return f, n, z, c, far, near, ups, (x, y, z, 1 - c)


def landed(pieces, pack, sem):
    part = pack.at[pl.ds(0, pieces)]
    pltpu.make_async_copy(part, part, sem).wait()


def gather_copies(k, stage, pack, whole, sent, came):
    f, n, z, c, far, near, ups, twin = route(k)
    every, z_first = slice(None), k % 3 < 2

    def go(i, where, *at):
        part = whole.at[(k,) + at]
        return send(part, part, (sent.at[0], came.at[k, i]), where)

    def own(i, where):
        return send(pack.at[k], whole.at[k, f, n, z, c], (sent.at[1], came.at[k, i]), where)

    if stage == 0:
        return [own(0, up) for up in ups] if z_first else [own(1, near)]
    if stage == 1:
        return [go(1, near, f, n, every, c)] if z_first else [go(0, up, f, every, z, c) for up in ups]
    if stage == 2:
        return [go(2, far, f, every, every, c)]
    return [go(3, twin, every, every, every, c)]


def gather_tick(t, bufs):
    pack, came = bufs[0], bufs[3]
    for stage in (4, 3, 2, 1, 0):
        k = t - GATHER_AT[stage]
        if not 0 <= k < CHUNKS:
            continue
        z_first = k % 3 < 2
        if stage == 1:
            landed(3 if z_first else 1, pack, came.at[k, 0 if z_first else 1])
        if stage == 2:
            landed(4 if z_first else 6, pack, came.at[k, 1 if z_first else 0])
        if stage == 3:
            landed(8, pack, came.at[k, 2])
        if stage == 4:
            landed(16, pack, came.at[k, 3])
        else:
            for copy in gather_copies(k, stage, *bufs):
                copy.start()


SUM_AT = (0, 1, 4, 7, 9)


def wide(ref, *at):
    return ref[at].astype(F32)


def sum_stages(k, own, fromtwin, fromfar, fromnear, fromz, sems, out, squares, put):
    f, n, z, c, far, near, ups, twin = route(k)
    slot, mine, zs = mod(k, SLOTS), mod(k, OWN), mod(k, FROMZ)
    every = slice(None)

    def pair(i):
        return sems.at[slot, 5], sems.at[slot, 1 + i]

    def two(*at):
        return wide(own, mine, *at) + wide(fromtwin, slot, *at)

    def to_twin():
        return send(own.at[OWN + mod(k, OTHER)], fromtwin.at[slot], (sems.at[slot, 0], sems.at[slot, 1]), twin)

    def to_far():
        return send(fromtwin.at[slot, 1 - f], fromfar.at[slot], pair(1), far)

    def first():
        to_twin().start()

    def second():
        to_twin().wait()

        def add(i, _):
            at = (1 - f, i // 2, pl.ds(2 * (i % 2), 2))
            fromtwin[(slot,) + at] = two(*at).astype(BF)
            return 0

        lax.fori_loop(0, 4, add, 0)
        to_far().start()

    def near_first():
        return send(fromtwin.at[slot, f, 1 - n], fromnear.at[slot], pair(2), near)

    def z_last(hop):
        to = ups[hop][2]
        return send(fromtwin.at[slot, f, n, to], fromz.at[zs, hop, 0], pair(3), ups[hop])

    def third_near():
        to_far().wait_recv()

        def add(i, _):
            at = (1 - n, pl.ds(2 * i, 2))
            fromtwin[(slot, f) + at] = (two(f, *at) + wide(fromfar, slot, *at)).astype(BF)
            return 0

        lax.fori_loop(0, 2, add, 0)
        near_first().start()

    def fourth_near():
        near_first().wait_recv()
        for hop in range(3):
            to = ups[hop][2]
            total = two(f, n, to) + wide(fromfar, slot, n, to) + wide(fromnear, slot, to)
            fromtwin[slot, f, n, to] = total.astype(BF)
            z_last(hop).start()

    def fifth_near():
        landed(3, out, sems.at[slot, 4])
        return wide(fromnear, slot, z) + wide(fromz, zs, 0, 0) + wide(fromz, zs, 1, 0) + wide(fromz, zs, 2, 0)

    def z_first(hop):
        to = ups[hop][2]
        return send(fromtwin.at[slot, f, every, to], fromz.at[zs, hop], pair(3), ups[hop])

    def near_last():
        return send(fromtwin.at[slot, f, 1 - n, z], fromnear.at[slot, 0], pair(2), near)

    def third_z():
        to_far().wait_recv()
        for hop in range(3):
            to = ups[hop][2]
            for i in range(2):
                fromtwin[slot, f, i, to] = (two(f, i, to) + wide(fromfar, slot, i, to)).astype(BF)
            z_first(hop).start()

    def along_z(i):
        return wide(fromz, zs, 0, i) + wide(fromz, zs, 1, i) + wide(fromz, zs, 2, i)

    def fourth_z():
        landed(6, out, sems.at[slot, 4])
        total = two(f, 1 - n, z) + wide(fromfar, slot, 1 - n, z) + along_z(1 - n)
        fromtwin[slot, f, 1 - n, z] = total.astype(BF)
        near_last().start()

    def fifth_z():
        near_last().wait_recv()
        return along_z(n) + wide(fromnear, slot, 0)

    def fifth(rest):
        landed(15, out, sems.at[slot, 5])
        total = (two(f, n, z) + wide(fromfar, slot, n, z) + rest()).astype(BF)
        out[k] = total
        put(k)
        square = total.astype(F32)
        square = square * square
        squares[...] += jnp.sum(square.reshape(16, 8, 128), axis=0)

    def last_near():
        fifth(fifth_near)

    def last_z():
        fifth(fifth_z)

    return (first, second, (third_near, third_z), (fourth_near, fourth_z), (last_near, last_z))


def sum_tick(t, bufs):
    for stage in (4, 3, 2, 1, 0):
        k = t - SUM_AT[stage]

        @pl.when(jnp.logical_and(k >= 0, k < CHUNKS))
        def _():
            if stage < 2:
                sum_stages(k, *bufs)[stage]()
            else:
                pl.when(mod(k, 3) < 2)(lambda: sum_stages(k, *bufs)[stage][0]())
                pl.when(mod(k, 3) >= 2)(lambda: sum_stages(k, *bufs)[stage][1]())


def corners():
    x, y, z, c = place()
    return [(x ^ (i // 4), y ^ (i // 2 % 2), z, c ^ (i % 2)) for i in range(1, 8)]


def all_squares(squares, total, box, sems):
    x, y, z, c = place()
    for at, others in ((0, corners()), (8, [(x, y, (z + hop) & 3, c) for hop in (1, 2, 3)])):
        box[at] = jnp.broadcast_to(jnp.sum(squares[...]), (8, 128)) if at == 0 else sum(box[i] for i in range(8))
        for i, other in enumerate(others):
            send(box.at[at], box.at[at + 1 + i], (sems.at[0, at // 8], sems.at[1, at // 8]), other).start()
        some = box.at[pl.ds(at + 1, len(others))]
        for i in range(2):
            pltpu.make_async_copy(some, some, sems.at[i, at // 8]).wait()
    total[0, 0] = jnp.max(sum(box[i] for i in range(8, 12)))


NN, NT, TN = (((1,), (0,)), ((), ())), (((1,), (1,)), ((), ())), (((0,), (0,)), ((), ()))


def dot(a, b, dims):
    return lax.dot_general(a, b, dims, preferred_element_type=F32)


def loop(n, body):
    lax.fori_loop(0, n, lambda i, _: (body(i), 0)[1], 0)


def rows(i):
    return pl.ds(pl.multiple_of(i * 1024, 1024), 1024)


def half(i):
    return pl.ds(pl.multiple_of(i * 512, 512), 512)


def spots(k, rail, c, b):
    same = 1 - (rail - c) * (rail - c)
    at = same * mod(k, OWN) + (1 - same) * (OWN + mod(k, OTHER))
    color, bx, by = mod(k, 2), div(b, 2), mod(b, 2)
    return at, bx + color * (by - bx), by + color * (bx - by)


def keep_wide(own, k, r, c):
    for b in range(4):
        for j in range(4):
            part = r[256 * b : 256 * b + 256, 128 * j : 128 * j + 128].astype(BF).reshape(4, 2, 32, 128)
            for rail in range(2):
                at, far, near = spots(k, rail, c, b)
                own[at, far, near, :, j] = part[:, rail]


def keep_tall(own, k, b, r, c):
    part = r.astype(BF).reshape(4, 2, 4, 32, 128)
    for rail in range(2):
        at, far, near = spots(k, rail, c, b)
        own[at, far, near] = part[:, rail]


def step_kernel(*refs):
    (x_in, dy_in), shards = [ref.at[0] for ref in refs[0:2]], refs[2:5]
    total, grads, whole = refs[5], refs[6:9], refs[9]
    acts, silus, slopes, douts, h1, a0 = refs[10:16]
    A, B, D, W, F, S, pack, own, fromtwin, fromfar, fromnear, fromz, squares, box = refs[16:30]
    gsems, glocal, ssems, last, load, tiles = refs[30:36]
    find()
    x, y, z, c = place()
    copy = pltpu.make_async_copy

    def packed(k):
        if 16 <= k < 32:
            return [copy(shards[2].at[k // 24].reshape(4, 32, 1024).at[:, :, pl.ds(k % 8 * 128, 128)], pack.at[k], glocal.at[0])]
        first = (k % 32) // 4 * 1024 + (k % 4) // 2 * 512
        return [copy(shards[k % 2].at[k // 32, :, pl.ds(first + 128 * j, 128)], pack.at[k, j], glocal.at[0]) for j in range(4)]

    for k in range(CHUNKS):
        for one in packed(k):
            one.start()
    copy(x_in, D.at[0], load.at[0]).start()
    copy(dy_in, B, load.at[1]).start()
    squares[...] = jnp.zeros_like(squares)
    greet()
    copy(pack, pack, glocal.at[0]).wait()

    def sent_all(i):
        first = sum(3 if k % 3 < 2 else 1 for k in range(CHUNKS))
        part = whole.reshape(32 * CHUNKS, 4, 32, 128).at[pl.ds(0, first if i else 31 * CHUNKS - first)]
        copy(part, part, glocal.at[2 + i]).wait()

    def put(k):
        n, first = 1 - div(k, 24), div(mod(k, 32), 4) * 1024 + mod(k, 2) * 512
        flat = jnp.logical_or(k < 16, k >= 32)
        for i in range(2):

            @pl.when(jnp.logical_and(flat, div(mod(k, 4), 2) == i))
            def _():
                for j in range(4):
                    cut = pl.ds(pl.multiple_of(first + 128 * j, 128), 128)
                    copy(pack.at[k, j], grads[i].at[n, :, cut], glocal.at[0]).start()

        @pl.when(jnp.logical_not(flat))
        def _():
            cut = pl.ds(pl.multiple_of(mod(k, 8) * 128, 128), 128)
            copy(pack.at[k], grads[2].at[n].reshape(4, 32, 1024).at[:, :, cut], glocal.at[0]).start()

    bufs = (own, fromtwin, fromfar, fromnear, fromz, ssems, pack, squares, put)

    def tick(t):
        gather_tick(t, (pack, whole, glocal.at[pl.ds(2, 2)], gsems))

    def ticks_at(step, first, count, every=1):
        for i in range(count):
            pl.when(step == i * every)(lambda i=i: tick(first + i))

    def sum_at(when, t):
        pl.when(when)(lambda: sum_tick(t, bufs))

    tick(0)
    tick(1)
    for k in range(CHUNKS):
        f, n = route(k)[:2]
        copy(pack.at[k], whole.at[k, f, n, z, c], glocal.at[1]).start()
    copy(pack, pack, glocal.at[1]).wait()
    tick(2)
    tick(3)
    copy(x_in, D.at[0], load.at[0]).wait()

    def norm(h):
        wide_h = h.astype(F32)
        return (wide_h * lax.rsqrt(jnp.mean(wide_h * wide_h, -1, keepdims=True) + 1e-6)).astype(BF)

    def first_norm(i):
        at = pl.ds(pl.multiple_of(i * 128, 128), 128)
        A[at] = norm(D[0, at])

    loop(16, first_norm)
    copy(A, a0, load.at[0]).start()
    for t in range(DONE):
        tick(4 + t)
    copy(A, a0, load.at[0]).wait()

    def wide_half(n, q, h):
        def part(blk):
            bx, by = div(blk, 2), mod(blk, 2)
            for i in range(2):
                k = 32 * n + 4 * q + 2 * h + i
                for j in range(4):
                    cut = pl.ds(512 * h + 128 * j, 128)
                    src = whole.at[k, bx + i * (by - bx), by + i * (bx - by), :, :, j]
                    copy(src, W.at[i].reshape(4, 4, 2, 32, 1024).at[blk, :, :, :, cut], load.at[2 + h]).start()

        loop(4, part)

    def half_loaded(h):
        part = W.at[:, :, pl.ds(512 * h, 512)]
        copy(part, part, load.at[2 + h]).wait()

    def tall_quarter(n, q, b):
        def part(j):
            color, bx, by = j % 2, q // 2, q % 2
            cut = pl.ds(pl.multiple_of(128 * j, 128), 128)
            src = whole.at[16 + 8 * n + j, bx + color * (by - bx), by + color * (bx - by)]
            copy(src, W.at[b].reshape(4, 2, 4, 32, 1024).at[:, :, :, :, cut], load.at[2 + b]).start()

        loop(8, part)

    def loaded(b):
        copy(W.at[b], W.at[b], load.at[2 + b]).wait()

    def phase_gu0():
        def gate_up_0(q):
            b = q % 2

            @pl.when(q >= 2)
            def _():
                copy(D.at[b], acts.at[0, q - 2], load.at[4 + b]).wait()

            def tile(i):
                for j in range(16):
                    pl.when(4 * q + i == j)(lambda j=j: tick(DONE + 4 + 5 * (j // 4) + (0, 1, 3, 4)[j % 4]))
                n, m, e = i // 2, i % 2, i % 2

                @pl.when(i == 0)
                def _():
                    wide_half(0, q, 1)
                    half_loaded(0)

                @pl.when(i == 2)
                def _():
                    half_loaded(1)
                    pl.when(q < 3)(lambda: wide_half(0, q + 1, 0))

                number_of = 4 * q + i

                @pl.when(number_of >= 2)
                def _():
                    copy(F.at[e], silus.at[number_of - 2], tiles.at[0, e]).wait()
                    copy(F.at[2 + e], slopes.at[number_of - 2], tiles.at[1, e]).wait()

                def part(j):
                    for at in range(4):
                        pl.when(jnp.logical_and(q == at, 2 * i + j == 3))(lambda at=at: tick(DONE + 6 + 5 * at))
                    here = half(j)
                    there = pl.ds(pl.multiple_of(m * 1024 + j * 512, 512), 512)
                    gate = dot(A[there], W[0, :, half(n)], NN)
                    up = dot(A[there], W[1, :, half(n)], NN)
                    s = jax.nn.sigmoid(gate)
                    silu = gate * s
                    F[e, here] = silu
                    F[2 + e, here] = up * (s + silu * (1 - s))
                    D[b, there, half(n)] = (silu * up).astype(BF)

                loop(2, part)
                copy(F.at[e], silus.at[number_of], tiles.at[0, e]).start()
                copy(F.at[2 + e], slopes.at[number_of], tiles.at[1, e]).start()

            loop(4, tile)
            copy(D.at[b], acts.at[0, q], load.at[4 + b]).start()

        wide_half(0, 0, 0)
        loop(4, gate_up_0)
        for e in range(2):
            copy(F.at[e], silus.at[14 + e], tiles.at[0, e]).wait()
            copy(F.at[2 + e], slopes.at[14 + e], tiles.at[1, e]).wait()
            copy(D.at[e], acts.at[0, 2 + e], load.at[4 + e]).wait()

    phase_gu0()

    def act_quarter(n, q, b):
        return copy(acts.at[n, q], D.at[b], load.at[4 + b])

    def phase_down0():
        tall_quarter(0, 0, 0)
        act_quarter(0, 0, 0).start()

        def down_0(q):
            b = q % 2
            loaded(b)
            act_quarter(0, q, b).wait()

            @pl.when(q < 3)
            def _():
                tall_quarter(0, q + 1, 1 - b)
                act_quarter(0, q + 1, 1 - b).start()

            def tile(i):
                ticks_at(4 * q + i, DONE + 24, 8, 2)
                m, n = i // 2, i % 2
                part = dot(D[b, rows(m)], W[b, :, half(n)], NN)

                @pl.when(q == 0)
                def _():
                    F[i] = part

                @pl.when(q > 0)
                def _():
                    F[i] += part

            loop(4, tile)

        loop(4, down_0)

    phase_down0()
    copy(x_in, D.at[0], load.at[0]).start()
    copy(dy_in, B, load.at[1]).wait()
    copy(x_in, D.at[0], load.at[0]).wait()

    def phase_norm2():
        def second_norm(i):
            at = pl.ds(pl.multiple_of(i * 128, 128), 128)
            m, r = i // 8, pl.ds(pl.multiple_of(i % 8 * 128, 128), 128)
            for n in range(2):
                cut = pl.ds(512 * n, 512)
                D[1, at, cut] = (D[0, at, cut].astype(F32) + F[2 * m + n, r].astype(BF).astype(F32)).astype(BF)
            A[at] = norm(D[1, at])

        loop(16, second_norm)

    phase_norm2()
    copy(D.at[1], h1, load.at[0]).start()

    def phase_hid1():
        tall_quarter(1, 0, 0)

        def by_hidden_1(q):
            b = q % 2
            loaded(b)

            @pl.when(q < 3)
            def _():
                tall_quarter(1, q + 1, 1 - b)

            def tile(i):
                ticks_at(4 * q + i, DONE + 32, 6, 3)
                n, m, e = i // 2, i % 2, i % 2
                number_of = 4 * q + i

                @pl.when(number_of >= 2)
                def _():
                    copy(S.at[e], douts.at[number_of - 2], tiles.at[0, e]).wait()

                S[e] = dot(B[rows(m)], W[b, half(n)], NT).astype(BF)
                copy(S.at[e], douts.at[number_of], tiles.at[0, e]).start()

            loop(4, tile)

        loop(4, by_hidden_1)
        for e in range(2):
            copy(S.at[e], douts.at[14 + e], tiles.at[0, e]).wait()

    phase_hid1()
    copy(D.at[1], h1, load.at[0]).wait()

    def wide_gradient(k, i):
        for n in range(2):
            keep_wide(own, k + 2 * i + n, dot(A[...], D[i, :, pl.ds(512 * n, 512)], TN), c)

    def phase_l1():
        wide_half(1, 0, 0)
        wide_half(1, 0, 1)

        def layer_1(q):
            half_loaded(0)
            pl.when(q == 1)(lambda: sent_all(1))
            copy(douts.at[4 * q], S.at[0], tiles.at[0, 0]).start()

            def tile(i):
                for j in range(6):
                    pl.when(4 * q + i == 4 * (j // 2) + 2 * (j % 2) + 1)(lambda j=j: tick(DONE + 38 + 4 * (j // 2) + j % 2))
                sum_at(i % 2 == 0, 4 * q + i // 2 - 3)
                n, m, e = i // 2, i % 2, i % 2
                pl.when(i == 2)(lambda: half_loaded(1))
                number_of = 4 * q + i
                copy(douts.at[number_of], S.at[e], tiles.at[0, e]).wait()

                @pl.when(i < 3)
                def _():
                    copy(douts.at[number_of + 1], S.at[1 - e], tiles.at[0, 1 - e]).start()

                @pl.when(number_of >= 2)
                def _():
                    copy(S.at[2 + e], acts.at[1, q, rows(m), half(n)], tiles.at[1, e]).wait()

                def part(j):
                    here = pl.ds(pl.multiple_of(j * 512, 512), 512)
                    there = pl.ds(pl.multiple_of(m * 1024 + j * 512, 512), 512)
                    gate = dot(A[there], W[0, :, half(n)], NN)
                    up = dot(A[there], W[1, :, half(n)], NN)
                    by_act = S[e, here].astype(F32)
                    s = jax.nn.sigmoid(gate)
                    silu = gate * s
                    S[2 + e, here] = (silu * up).astype(BF)
                    D[1, there, half(n)] = (by_act * silu).astype(BF)
                    D[0, there, half(n)] = (by_act * (up * (s + silu * (1 - s)))).astype(BF)

                loop(1024 // 512, part)
                copy(S.at[2 + e], acts.at[1, q, rows(m), half(n)], tiles.at[1, e]).start()

            loop(4, tile)

            def back(m):
                for j in range(3):
                    pl.when(jnp.logical_and(q == j, m == 1))(lambda j=j: tick(DONE + 40 + 4 * j))
                sum_at(m == 0, 4 * q - 1)
                for n in range(2):
                    cut = pl.ds(512 * n, 512)
                    part = dot(D[0, rows(m)], W[0, cut], NT) + dot(D[1, rows(m)], W[1, cut], NT)
                    F[2 * m + n] = jnp.where(q > 0, F[2 * m + n], 0) + part

            loop(2, back)

            def part(i):
                for j in range(2):
                    pl.when(jnp.logical_and(q == j, i == 1))(lambda j=j: tick(DONE + 41 + 4 * j))

                for h in range(2):
                    pl.when(jnp.logical_and(q < 3, i == h))(lambda h=h: wide_half(1, q + 1, h))
                wide_gradient(4 * q, i)
                sum_at(i == 0, 4 * q)

            loop(2, part)

        loop(4, layer_1)
        for e in range(2):
            copy(S.at[2 + e], acts.at[1, 3, rows(1), half(e)], tiles.at[1, e]).wait()


    phase_l1()
    sent_all(0)
    def tall_part(b, k, i):
        p, q = i // 4, i % 4
        r = dot(D[b], B[:, half(p)], TN)
        for j in range(4):
            keep_tall(own, k + 4 * p + j, q, r[:, 128 * j : 128 * j + 128], c)

    def tall_gradient(n, k, t, places):
        act_quarter(n, 0, 0).start()

        def part(i):
            b = i % 2
            act_quarter(n, i % 4, b).wait()
            pl.when(i < 7)(lambda: act_quarter(n, (i + 1) % 4, 1 - b).start())
            tall_part(b, k, i)
            sum_at(sum((i == p).astype(jnp.int32) for p in places) > 0, t + sum((i > p).astype(jnp.int32) for p in places))

        loop(8, part)

    tall_gradient(1, 16, 13, (0, 1, 3, 4, 6, 7))

    copy(h1, D.at[0], load.at[0]).start()
    copy(a0, A, load.at[1]).start()
    copy(h1, D.at[0], load.at[0]).wait()

    def phase_nback():
        def norm_back(i):
            at = pl.ds(pl.multiple_of(i * 128, 128), 128)
            m, r = i // 8, pl.ds(pl.multiple_of(i % 8 * 128, 128), 128)
            h = D[0, at].astype(F32)
            scale = lax.rsqrt(jnp.mean(h * h, -1, keepdims=True) + 1e-6)
            by_a = [F[2 * m + n, r].astype(BF).astype(F32) for n in range(2)]
            parts = [h[:, 512 * n : 512 * n + 512] for n in range(2)]
            along = sum(jnp.sum(one * part, -1, keepdims=True) for one, part in zip(by_a, parts, strict=True))
            along = along * (scale * scale * scale) * (1 / 1024)
            for n in range(2):
                cut = pl.ds(512 * n, 512)
                by_h = (by_a[n] * scale - parts[n] * along).astype(BF)
                B[at, cut] = (B[at, cut].astype(F32) + by_h.astype(F32)).astype(BF)

        loop(16, norm_back)

    sum_tick(19, bufs)
    phase_nback()
    sum_tick(20, bufs)
    tall_gradient(0, 24, 21, (0, 1, 3, 5, 7))

    def kept_tile(number_of, e):
        return (
            copy(silus.at[number_of], F.at[e], tiles.at[0, e]),
            copy(slopes.at[number_of], F.at[2 + e], tiles.at[1, e]),
        )

    copy(a0, A, load.at[1]).wait()
    def phase_l0():
        tall_quarter(0, 0, 0)
        for one in kept_tile(0, 0):
            one.start()

        def layer_0(q):
            b = q % 2
            loaded(b)

            @pl.when(q < 3)
            def _():
                tall_quarter(0, q + 1, 1 - b)

            def tile(i):
                sum_at(i != 1, 26 + 5 * q + i // 2 + i // 3)
                n, m, e = i // 2, i % 2, i % 2
                number_of = 4 * q + i
                for one in kept_tile(number_of, e):
                    one.wait()

                @pl.when(number_of < 15)
                def _():
                    for one in kept_tile(number_of + 1, 1 - e):
                        one.start()

                for part in range(2):
                    here = pl.ds(512 * part, 512)
                    there = pl.ds(pl.multiple_of(m * 1024 + 512 * part, 512), 512)
                    by_act = dot(B[there], W[b, half(n)], NT).astype(BF).astype(F32)
                    D[1, there, half(n)] = (by_act * F[e, here]).astype(BF)
                    D[0, there, half(n)] = (by_act * F[2 + e, here]).astype(BF)

            loop(4, tile)
            def part(i):
                sum_at(jnp.logical_or(i == 1, i == 2), 28 + 5 * q + i)
                keep_wide(own, 32 + 4 * q + i, dot(A[...], D[i // 2, :, half(i % 2)], TN), c)

            loop(4, part)

        loop(4, layer_0)

    phase_l0()
    loop(SUM_AT[-1] + 2, lambda t: sum_tick(CHUNKS - 2 + t, bufs))
    all_squares(squares, total, box, last)
    copy(pack, pack, glocal.at[0]).wait()


def stepped(x, dy, weights):
    block, hbm, shape = (4, 32, 128), pl.BlockSpec(memory_space=pl.ANY), jax.ShapeDtypeStruct
    results = pl.pallas_call(
        step_kernel,
        name="step",
        out_shape=[shape((1, 1), F32)]
        + [shape(w.shape, BF) for w in weights]
        + [
            shape((CHUNKS, 2, 2, 4, 2) + block, BF),
            shape((2, 4, 2048, 1024), BF),
            shape((16, 1024, 512), F32),
            shape((16, 1024, 512), F32),
            shape((16, 1024, 512), BF),
            shape((2048, 1024), BF),
            shape((2048, 1024), BF),
        ],
        in_specs=[hbm] * 5,
        out_specs=[pl.BlockSpec(memory_space=pltpu.SMEM)] + [hbm] * 10,
        scratch_shapes=[
            pltpu.VMEM((2048, 1024), BF),
            pltpu.VMEM((2048, 1024), BF),
            pltpu.VMEM((2, 2048, 1024), BF),
            pltpu.VMEM((2, 1024, 1024), BF),
            pltpu.VMEM((4, 1024, 512), F32),
            pltpu.VMEM((4, 1024, 512), BF),
            pltpu.VMEM((CHUNKS,) + block, BF),
            pltpu.VMEM((OWN + OTHER, 2, 2, 4) + block, BF),
            pltpu.VMEM((SLOTS, 2, 2, 4) + block, BF),
            pltpu.VMEM((SLOTS, 2, 4) + block, BF),
            pltpu.VMEM((SLOTS, 4) + block, BF),
            pltpu.VMEM((FROMZ, 3, 2) + block, BF),
            pltpu.VMEM((8, 128), F32),
            pltpu.VMEM((12, 8, 128), F32),
            pltpu.SemaphoreType.DMA((CHUNKS, 4)),
            pltpu.SemaphoreType.DMA((4,)),
            pltpu.SemaphoreType.DMA((SLOTS, 6)),
            pltpu.SemaphoreType.DMA((2, 2)),
            pltpu.SemaphoreType.DMA((6,)),
            pltpu.SemaphoreType.DMA((2, 2)),
        ],
        compiler_params=pltpu.CompilerParams(collective_id=0, has_side_effects=True, vmem_limit_bytes=67043328),
    )(x, dy, *weights)
    return results[0], results[1:4]


def solution(mesh):
    def step(x, dy, *arrays):
        weights, m, v = (arrays[i : i + 3] for i in (0, 3, 6))
        squares, mine = stepped(x, dy, weights)
        count = 32 * sum(g.size for g in mine)
        factor = jnp.minimum(1.0, 0.5 * lax.rsqrt(squares[0, 0] / count + 1e-30))
        new = [adamw(w.astype(F32), m, v, g.astype(F32) * factor) for w, m, v, g in zip(weights, m, v, mine, strict=True)]
        return tuple(one[which] for which in range(3) for one in new)

    states, cut = P(("rep", "dp"), None, None), P(None, "dp", None)
    return jax.shard_map(
        step,
        mesh=mesh,
        in_specs=(states, states) + (cut,) * 9,
        out_specs=(P("rep", "dp", None),) * 9,
        check_vma=False,
    )
```

```python
import jax
import jax.numpy as jnp
from jax import lax
from jax.experimental import pallas as pl
from jax.experimental.pallas import tpu as pltpu
from jax.sharding import PartitionSpec as P

BF, F32 = jnp.bfloat16, jnp.float32
MESH = pl.DeviceIdType.MESH
CHUNKS = 48
SLOTS, OWN, OTHER, FROMZ = 12, 17, 9, 9


def adamw(w, m, v, g):
    m = 0.9 * m + 0.1 * g
    v = 0.95 * v + 0.05 * g * g
    step = m * lax.rsqrt(v + 1e-8) + 0.1 * w
    return (w - 0.02 * step).astype(jnp.bfloat16), m, v


HERE = []


def find():
    me = lax.axis_index("dp")
    HERE[:] = [lax.div(me, 16), lax.rem(lax.div(me, 8), 2), lax.rem(lax.div(me, 2), 4), lax.rem(me, 2)]


def place():
    return tuple(HERE)


def mod(a, b):
    return a % b if isinstance(a, int) else lax.rem(a, b)


def div(a, b):
    return a // b if isinstance(a, int) else lax.div(a, b)


def number(x, y, z, c):
    return ((x * 2 + y) * 4 + z) * 2 + c


def greet():
    x, y, z, c = place()
    barrier = pltpu.get_barrier_semaphore()
    others = corners()
    others += [(x, y, (z + hop) % 4, c) for hop in (1, 2, 3)]
    for other in others:
        pl.semaphore_signal(barrier, 1, device_id={"dp": number(*other)}, device_id_type=MESH)


def greeted():
    pl.semaphore_wait(pltpu.get_barrier_semaphore(), 10)


def send(src, dst, sems, where):
    return pltpu.make_async_remote_copy(
        src_ref=src, dst_ref=dst, send_sem=sems[0], recv_sem=sems[1], device_id={"dp": number(*where)}, device_id_type=MESH
    )


GATHER_AT = (0, 3, 5, 7, 8)
DONE = GATHER_AT[-1]


def route(k):
    x, y, z, c = place()
    color = mod(k, 2)
    f, n = x + color * (y - x), y + color * (x - y)
    far = (x + (1 - color) * (1 - 2 * x), y + color * (1 - 2 * y), z, c)
    near = (x + color * (1 - 2 * x), y + (1 - color) * (1 - 2 * y), z, c)
    ups = [(x, y, (z + hop) & 3, c) for hop in (1, 3, 2)]
    return f, n, z, c, far, near, ups, (x, y, z, 1 - c)


def landed(pieces, pack, sem):
    part = pack.at[pl.ds(0, pieces)]
    pltpu.make_async_copy(part, part, sem).wait()


def gather_copies(k, stage, pack, whole, sent, came):
    f, n, z, c, far, near, ups, twin = route(k)
    every, z_first = slice(None), k % 3 < 2

    def go(i, where, *at):
        part = whole.at[(k,) + at]
        return send(part, part, (sent.at[0], came.at[k, i]), where)

    def own(i, where):
        return send(pack.at[k], whole.at[k, f, n, z, c], (sent.at[1], came.at[k, i]), where)

    if stage == 0:
        return [own(0, up) for up in ups] if z_first else [own(1, near)]
    if stage == 1:
        return [go(1, near, f, n, every, c)] if z_first else [go(0, up, f, every, z, c) for up in ups]
    if stage == 2:
        return [go(2, far, f, every, every, c)]
    return [go(3, twin, every, every, every, c)]


def gather_tick(t, bufs):
    pack, came = bufs[0], bufs[3]
    for stage in (4, 3, 2, 1, 0):
        k = t - GATHER_AT[stage]
        if not 0 <= k < CHUNKS:
            continue
        z_first = k % 3 < 2
        if stage == 1:
            landed(3 if z_first else 1, pack, came.at[k, 0 if z_first else 1])
        if stage == 2:
            landed(4 if z_first else 6, pack, came.at[k, 1 if z_first else 0])
        if stage == 3:
            landed(8, pack, came.at[k, 2])
        if stage == 4:
            landed(16, pack, came.at[k, 3])
        else:
            for copy in gather_copies(k, stage, *bufs):
                copy.start()


SUM_AT = (0, 1, 4, 7, 9)


def wide(ref, *at):
    return ref[at].astype(F32)


def sum_stages(k, own, fromtwin, fromfar, fromnear, fromz, sems, out, squares, put):
    f, n, z, c, far, near, ups, twin = route(k)
    slot, mine, zs = mod(k, SLOTS), mod(k, OWN), mod(k, FROMZ)
    every = slice(None)

    def pair(i):
        return sems.at[slot, 5], sems.at[slot, 1 + i]

    def two(*at):
        return wide(own, mine, *at) + wide(fromtwin, slot, *at)

    def to_twin():
        return send(own.at[OWN + mod(k, OTHER)], fromtwin.at[slot], (sems.at[slot, 0], sems.at[slot, 1]), twin)

    def to_far():
        return send(fromtwin.at[slot, 1 - f], fromfar.at[slot], pair(1), far)

    def first():
        to_twin().start()

    def second():
        to_twin().wait()

        def add(i, _):
            at = (1 - f, i // 2, pl.ds(2 * (i % 2), 2))
            fromtwin[(slot,) + at] = two(*at).astype(BF)
            return 0

        lax.fori_loop(0, 4, add, 0)
        to_far().start()

    def near_first():
        return send(fromtwin.at[slot, f, 1 - n], fromnear.at[slot], pair(2), near)

    def z_last(hop):
        to = ups[hop][2]
        return send(fromtwin.at[slot, f, n, to], fromz.at[zs, hop, 0], pair(3), ups[hop])

    def third_near():
        to_far().wait_recv()

        def add(i, _):
            at = (1 - n, pl.ds(2 * i, 2))
            fromtwin[(slot, f) + at] = (two(f, *at) + wide(fromfar, slot, *at)).astype(BF)
            return 0

        lax.fori_loop(0, 2, add, 0)
        near_first().start()

    def fourth_near():
        near_first().wait_recv()
        for hop in range(3):
            to = ups[hop][2]
            total = two(f, n, to) + wide(fromfar, slot, n, to) + wide(fromnear, slot, to)
            fromtwin[slot, f, n, to] = total.astype(BF)
            z_last(hop).start()

    def fifth_near():
        landed(3, out, sems.at[slot, 4])
        return wide(fromnear, slot, z) + wide(fromz, zs, 0, 0) + wide(fromz, zs, 1, 0) + wide(fromz, zs, 2, 0)

    def z_first(hop):
        to = ups[hop][2]
        return send(fromtwin.at[slot, f, every, to], fromz.at[zs, hop], pair(3), ups[hop])

    def near_last():
        return send(fromtwin.at[slot, f, 1 - n, z], fromnear.at[slot, 0], pair(2), near)

    def third_z():
        to_far().wait_recv()
        for hop in range(3):
            to = ups[hop][2]
            for i in range(2):
                fromtwin[slot, f, i, to] = (two(f, i, to) + wide(fromfar, slot, i, to)).astype(BF)
            z_first(hop).start()

    def along_z(i):
        return wide(fromz, zs, 0, i) + wide(fromz, zs, 1, i) + wide(fromz, zs, 2, i)

    def fourth_z():
        landed(6, out, sems.at[slot, 4])
        total = two(f, 1 - n, z) + wide(fromfar, slot, 1 - n, z) + along_z(1 - n)
        fromtwin[slot, f, 1 - n, z] = total.astype(BF)
        near_last().start()

    def fifth_z():
        near_last().wait_recv()
        return along_z(n) + wide(fromnear, slot, 0)

    def fifth(rest):
        landed(15, out, sems.at[slot, 5])
        total = (two(f, n, z) + wide(fromfar, slot, n, z) + rest()).astype(BF)
        out[k] = total
        put(k)
        square = total.astype(F32)
        square = square * square
        squares[...] += jnp.sum(square.reshape(16, 8, 128), axis=0)

    def last_near():
        fifth(fifth_near)

    def last_z():
        fifth(fifth_z)

    return (first, second, (third_near, third_z), (fourth_near, fourth_z), (last_near, last_z))


def sum_tick(t, bufs):
    for stage in (4, 3, 2, 1, 0):
        k = t - SUM_AT[stage]

        @pl.when(jnp.logical_and(k >= 0, k < CHUNKS))
        def _():
            if stage < 2:
                sum_stages(k, *bufs)[stage]()
            else:
                pl.when(mod(k, 3) < 2)(lambda: sum_stages(k, *bufs)[stage][0]())
                pl.when(mod(k, 3) >= 2)(lambda: sum_stages(k, *bufs)[stage][1]())


def corners():
    x, y, z, c = place()
    return [(x ^ (i // 4), y ^ (i // 2 % 2), z, c ^ (i % 2)) for i in range(1, 8)]


def all_squares(squares, total, box, sems):
    x, y, z, c = place()
    for at, others in ((0, corners()), (8, [(x, y, (z + hop) & 3, c) for hop in (1, 2, 3)])):
        box[at] = jnp.broadcast_to(jnp.sum(squares[...]), (8, 128)) if at == 0 else sum(box[i] for i in range(8))
        for i, other in enumerate(others):
            send(box.at[at], box.at[at + 1 + i], (sems.at[0, at // 8], sems.at[1, at // 8]), other).start()
        some = box.at[pl.ds(at + 1, len(others))]
        for i in range(2):
            pltpu.make_async_copy(some, some, sems.at[i, at // 8]).wait()
    total[0, 0] = jnp.max(sum(box[i] for i in range(8, 12)))


NN, NT, TN = (((1,), (0,)), ((), ())), (((1,), (1,)), ((), ())), (((0,), (0,)), ((), ()))


def dot(a, b, dims):
    return lax.dot_general(a, b, dims, preferred_element_type=F32)


def loop(n, body):
    lax.fori_loop(0, n, lambda i, _: (body(i), 0)[1], 0)


def rows(i):
    return pl.ds(pl.multiple_of(i * 1024, 1024), 1024)


def half(i):
    return pl.ds(pl.multiple_of(i * 512, 512), 512)


def spots(k, rail, c, b):
    same = 1 - (rail - c) * (rail - c)
    at = same * mod(k, OWN) + (1 - same) * (OWN + mod(k, OTHER))
    color, bx, by = mod(k, 2), div(b, 2), mod(b, 2)
    return at, bx + color * (by - bx), by + color * (bx - by)


def keep_wide(own, k, r, c):
    for b in range(4):
        for j in range(4):
            part = r[256 * b : 256 * b + 256, 128 * j : 128 * j + 128].astype(BF).reshape(4, 2, 32, 128)
            for rail in range(2):
                at, far, near = spots(k, rail, c, b)
                own[at, far, near, :, j] = part[:, rail]


def keep_tall(own, k, b, r, c):
    part = r.astype(BF).reshape(4, 2, 4, 32, 128)
    for rail in range(2):
        at, far, near = spots(k, rail, c, b)
        own[at, far, near] = part[:, rail]


def step_kernel(*refs):
    (x_in, dy_in), shards = [ref.at[0] for ref in refs[0:2]], refs[2:5]
    total, grads, whole = refs[5], refs[6:9], refs[9]
    acts, silus, slopes, douts, h1, a0 = refs[10:16]
    A, B, D, W, F, S, pack, own, fromtwin, fromfar, fromnear, fromz, squares, box = refs[16:30]
    gsems, glocal, ssems, last, load, tiles = refs[30:36]
    find()
    x, y, z, c = place()
    copy = pltpu.make_async_copy

    def packed(k):
        if 16 <= k < 32:
            return [copy(shards[2].at[k // 24].reshape(4, 32, 1024).at[:, :, pl.ds(k % 8 * 128, 128)], pack.at[k], glocal.at[0 if k > 3 else 4])]
        first = (k % 32) // 4 * 1024 + (k % 4) // 2 * 512
        return [copy(shards[k % 2].at[k // 32, :, pl.ds(first + 128 * j, 128)], pack.at[k, j], glocal.at[0 if k > 3 else 4]) for j in range(4)]

    greet()
    for k in range(CHUNKS):
        for one in packed(k):
            one.start()
    copy(x_in, D.at[0], load.at[0]).start()
    copy(dy_in, B, load.at[1]).start()
    squares[...] = jnp.zeros_like(squares)
    greeted()

    def sent_all(i):
        first = sum(3 if k % 3 < 2 else 1 for k in range(CHUNKS))
        part = whole.reshape(32 * CHUNKS, 4, 32, 128).at[pl.ds(0, first if i else 31 * CHUNKS - first)]
        copy(part, part, glocal.at[2 + i]).wait()

    def put(k):
        n, first = 1 - div(k, 24), div(mod(k, 32), 4) * 1024 + mod(k, 2) * 512
        flat = jnp.logical_or(k < 16, k >= 32)
        for i in range(2):

            @pl.when(jnp.logical_and(flat, div(mod(k, 4), 2) == i))
            def _():
                for j in range(4):
                    cut = pl.ds(pl.multiple_of(first + 128 * j, 128), 128)
                    copy(pack.at[k, j], grads[i].at[n, :, cut], glocal.at[0]).start()

        @pl.when(jnp.logical_not(flat))
        def _():
            cut = pl.ds(pl.multiple_of(mod(k, 8) * 128, 128), 128)
            copy(pack.at[k], grads[2].at[n].reshape(4, 32, 1024).at[:, :, cut], glocal.at[0]).start()

    bufs = (own, fromtwin, fromfar, fromnear, fromz, ssems, pack, squares, put)

    def tick(t):
        gather_tick(t, (pack, whole, glocal.at[pl.ds(2, 2)], gsems))

    def ticks_at(step, first, count, every=1):
        for i in range(count):
            pl.when(step == i * every)(lambda i=i: tick(first + i))

    def sum_at(when, t):
        pl.when(when)(lambda: sum_tick(t, bufs))

    landed(4, pack, glocal.at[4])
    tick(0)
    tick(1)
    landed(CHUNKS - 4, pack, glocal.at[0])
    for k in range(CHUNKS):
        f, n = route(k)[:2]
        copy(pack.at[k], whole.at[k, f, n, z, c], glocal.at[1]).start()
    tick(2)
    copy(pack, pack, glocal.at[1]).wait()
    tick(3)
    copy(x_in, D.at[0], load.at[0]).wait()

    def norm(h):
        wide_h = h.astype(F32)
        return (wide_h * lax.rsqrt(jnp.mean(wide_h * wide_h, -1, keepdims=True) + 1e-6)).astype(BF)

    def first_norm(i):
        at = pl.ds(pl.multiple_of(i * 128, 128), 128)
        A[at] = norm(D[0, at])

    loop(16, first_norm)
    copy(A, a0, load.at[0]).start()
    for t in range(DONE):
        tick(4 + t)
    copy(A, a0, load.at[0]).wait()

    def wide_half(n, q, h):
        def part(blk):
            bx, by = div(blk, 2), mod(blk, 2)
            for i in range(2):
                k = 32 * n + 4 * q + 2 * h + i
                for j in range(4):
                    cut = pl.ds(512 * h + 128 * j, 128)
                    src = whole.at[k, bx + i * (by - bx), by + i * (bx - by), :, :, j]
                    copy(src, W.at[i].reshape(4, 4, 2, 32, 1024).at[blk, :, :, :, cut], load.at[2 + h]).start()

        loop(4, part)

    def half_loaded(h):
        part = W.at[:, :, pl.ds(512 * h, 512)]
        copy(part, part, load.at[2 + h]).wait()

    def tall_quarter(n, q, b):
        def part(j):
            color, bx, by = j % 2, q // 2, q % 2
            cut = pl.ds(pl.multiple_of(128 * j, 128), 128)
            src = whole.at[16 + 8 * n + j, bx + color * (by - bx), by + color * (bx - by)]
            copy(src, W.at[b].reshape(4, 2, 4, 32, 1024).at[:, :, :, :, cut], load.at[2 + b]).start()

        loop(8, part)

    def loaded(b):
        copy(W.at[b], W.at[b], load.at[2 + b]).wait()

    def phase_gu0():
        def gate_up_0(q):
            b = q % 2

            @pl.when(q >= 2)
            def _():
                copy(D.at[b], acts.at[0, q - 2], load.at[4 + b]).wait()

            def tile(i):
                for j in range(16):
                    pl.when(4 * q + i == j)(lambda j=j: tick(DONE + 4 + 5 * (j // 4) + (0, 1, 3, 4)[j % 4]))
                n, m, e = i // 2, i % 2, i % 2

                @pl.when(i == 0)
                def _():
                    wide_half(0, q, 1)
                    half_loaded(0)

                @pl.when(i == 2)
                def _():
                    half_loaded(1)
                    pl.when(q < 3)(lambda: wide_half(0, q + 1, 0))

                number_of = 4 * q + i

                @pl.when(number_of >= 2)
                def _():
                    copy(F.at[e], silus.at[number_of - 2], tiles.at[0, e]).wait()
                    copy(F.at[2 + e], slopes.at[number_of - 2], tiles.at[1, e]).wait()

                def part(j):
                    for at in range(4):
                        pl.when(jnp.logical_and(q == at, 2 * i + j == 3))(lambda at=at: tick(DONE + 6 + 5 * at))
                    here = half(j)
                    there = pl.ds(pl.multiple_of(m * 1024 + j * 512, 512), 512)
                    gate = dot(A[there], W[0, :, half(n)], NN)
                    up = dot(A[there], W[1, :, half(n)], NN)
                    s = jax.nn.sigmoid(gate)
                    silu = gate * s
                    F[e, here] = silu
                    F[2 + e, here] = up * (s + silu * (1 - s))
                    D[b, there, half(n)] = (silu * up).astype(BF)

                loop(2, part)
                copy(F.at[e], silus.at[number_of], tiles.at[0, e]).start()
                copy(F.at[2 + e], slopes.at[number_of], tiles.at[1, e]).start()

            loop(4, tile)
            copy(D.at[b], acts.at[0, q], load.at[4 + b]).start()

        wide_half(0, 0, 0)
        loop(4, gate_up_0)
        for e in range(2):
            copy(F.at[e], silus.at[14 + e], tiles.at[0, e]).wait()
            copy(F.at[2 + e], slopes.at[14 + e], tiles.at[1, e]).wait()
            copy(D.at[e], acts.at[0, 2 + e], load.at[4 + e]).wait()

    phase_gu0()

    def act_quarter(n, q, b):
        return copy(acts.at[n, q], D.at[b], load.at[4 + b])

    def phase_down0():
        tall_quarter(0, 0, 0)
        act_quarter(0, 0, 0).start()

        def down_0(q):
            b = q % 2
            loaded(b)
            act_quarter(0, q, b).wait()

            @pl.when(q < 3)
            def _():
                tall_quarter(0, q + 1, 1 - b)
                act_quarter(0, q + 1, 1 - b).start()

            pl.when(q == 3)(lambda: copy(x_in, D.at[0], load.at[0]).start())

            def tile(i):
                ticks_at(4 * q + i, DONE + 24, 8, 2)
                m, n = i // 2, i % 2
                part = dot(D[b, rows(m)], W[b, :, half(n)], NN)

                @pl.when(q == 0)
                def _():
                    F[i] = part

                @pl.when(q > 0)
                def _():
                    F[i] += part

            loop(4, tile)

        loop(4, down_0)

    phase_down0()
    tall_quarter(1, 0, 0)
    copy(dy_in, B, load.at[1]).wait()
    copy(x_in, D.at[0], load.at[0]).wait()

    def phase_norm2():
        def second_norm(i):
            at = pl.ds(pl.multiple_of(i * 128, 128), 128)
            m, r = i // 8, pl.ds(pl.multiple_of(i % 8 * 128, 128), 128)
            for n in range(2):
                cut = pl.ds(512 * n, 512)
                D[1, at, cut] = (D[0, at, cut].astype(F32) + F[2 * m + n, r].astype(BF).astype(F32)).astype(BF)
            A[at] = norm(D[1, at])

        loop(16, second_norm)

    phase_norm2()
    copy(D.at[1], h1, load.at[0]).start()

    def phase_hid1():
        def by_hidden_1(q):
            b = q % 2
            loaded(b)

            @pl.when(q < 3)
            def _():
                tall_quarter(1, q + 1, 1 - b)

            def tile(i):
                ticks_at(4 * q + i, DONE + 32, 6, 3)
                n, m, e = i // 2, i % 2, i % 2
                number_of = 4 * q + i

                @pl.when(number_of >= 2)
                def _():
                    copy(S.at[e], douts.at[number_of - 2], tiles.at[0, e]).wait()

                S[e] = dot(B[rows(m)], W[b, half(n)], NT).astype(BF)
                copy(S.at[e], douts.at[number_of], tiles.at[0, e]).start()

            loop(4, tile)

        loop(4, by_hidden_1)
        for e in range(2):
            copy(S.at[e], douts.at[14 + e], tiles.at[0, e]).wait()

    phase_hid1()
    copy(D.at[1], h1, load.at[0]).wait()

    def wide_gradient(k, i):
        for n in range(2):
            keep_wide(own, k + 2 * i + n, dot(A[...], D[i, :, pl.ds(512 * n, 512)], TN), c)

    def phase_l1():
        wide_half(1, 0, 0)
        wide_half(1, 0, 1)

        def layer_1(q):
            half_loaded(0)
            pl.when(q == 1)(lambda: sent_all(1))
            copy(douts.at[4 * q], S.at[0], tiles.at[0, 0]).start()

            def tile(i):
                for j in range(6):
                    pl.when(4 * q + i == 4 * (j // 2) + 2 * (j % 2) + 1)(lambda j=j: tick(DONE + 38 + 4 * (j // 2) + j % 2))
                sum_at(i % 2 == 0, 4 * q + i // 2 - 3)
                n, m, e = i // 2, i % 2, i % 2
                pl.when(i == 2)(lambda: half_loaded(1))
                number_of = 4 * q + i
                copy(douts.at[number_of], S.at[e], tiles.at[0, e]).wait()

                @pl.when(i < 3)
                def _():
                    copy(douts.at[number_of + 1], S.at[1 - e], tiles.at[0, 1 - e]).start()

                @pl.when(number_of >= 2)
                def _():
                    copy(S.at[2 + e], acts.at[1, q, rows(m), half(n)], tiles.at[1, e]).wait()

                def part(j):
                    here = pl.ds(pl.multiple_of(j * 512, 512), 512)
                    there = pl.ds(pl.multiple_of(m * 1024 + j * 512, 512), 512)
                    gate = dot(A[there], W[0, :, half(n)], NN)
                    up = dot(A[there], W[1, :, half(n)], NN)
                    by_act = S[e, here].astype(F32)
                    s = jax.nn.sigmoid(gate)
                    silu = gate * s
                    S[2 + e, here] = (silu * up).astype(BF)
                    D[1, there, half(n)] = (by_act * silu).astype(BF)
                    D[0, there, half(n)] = (by_act * (up * (s + silu * (1 - s)))).astype(BF)

                loop(1024 // 512, part)
                copy(S.at[2 + e], acts.at[1, q, rows(m), half(n)], tiles.at[1, e]).start()

            loop(4, tile)

            def back(m):
                for j in range(3):
                    pl.when(jnp.logical_and(q == j, m == 1))(lambda j=j: tick(DONE + 40 + 4 * j))
                sum_at(m == 0, 4 * q - 1)
                for n in range(2):
                    cut = pl.ds(512 * n, 512)
                    part = dot(D[0, rows(m)], W[0, cut], NT) + dot(D[1, rows(m)], W[1, cut], NT)
                    F[2 * m + n] = jnp.where(q > 0, F[2 * m + n], 0) + part

            loop(2, back)

            def part(i):
                for j in range(2):
                    pl.when(jnp.logical_and(q == j, i == 1))(lambda j=j: tick(DONE + 41 + 4 * j))

                for h in range(2):
                    pl.when(jnp.logical_and(q < 3, i == h))(lambda h=h: wide_half(1, q + 1, h))
                pl.when(jnp.logical_and(q == 3, i == 1))(lambda: act_quarter(1, 0, 0).start())
                wide_gradient(4 * q, i)
                sum_at(i == 0, 4 * q)

            loop(2, part)

        loop(4, layer_1)
        for e in range(2):
            copy(S.at[2 + e], acts.at[1, 3, rows(1), half(e)], tiles.at[1, e]).wait()


    phase_l1()
    sent_all(0)
    def tall_part(b, k, i):
        p, q = i // 4, i % 4
        r = dot(D[b], B[:, half(p)], TN)
        for j in range(4):
            keep_tall(own, k + 4 * p + j, q, r[:, 128 * j : 128 * j + 128], c)

    def tall_gradient(n, k, t, places, at, then):
        def part(i):
            b = (i + at) % 2
            act_quarter(n, i % 4, b).wait()
            pl.when(i == 7)(then)
            pl.when(i < 7)(lambda: act_quarter(n, (i + 1) % 4, 1 - b).start())
            tall_part(b, k, i)
            sum_at(sum((i == p).astype(jnp.int32) for p in places) > 0, t + sum((i > p).astype(jnp.int32) for p in places))

        loop(8, part)

    copy(a0, A, load.at[1]).start()
    tall_gradient(1, 16, 13, (0, 1, 3, 4, 6, 7), 0, lambda: copy(h1, D.at[0], load.at[0]).start())

    act_quarter(0, 0, 1).start()
    copy(h1, D.at[0], load.at[0]).wait()

    def phase_nback():
        def norm_back(i):
            at = pl.ds(pl.multiple_of(i * 128, 128), 128)
            m, r = i // 8, pl.ds(pl.multiple_of(i % 8 * 128, 128), 128)
            h = D[0, at].astype(F32)
            scale = lax.rsqrt(jnp.mean(h * h, -1, keepdims=True) + 1e-6)
            by_a = [F[2 * m + n, r].astype(BF).astype(F32) for n in range(2)]
            parts = [h[:, 512 * n : 512 * n + 512] for n in range(2)]
            along = sum(jnp.sum(one * part, -1, keepdims=True) for one, part in zip(by_a, parts, strict=True))
            along = along * (scale * scale * scale) * (1 / 1024)
            for n in range(2):
                cut = pl.ds(512 * n, 512)
                by_h = (by_a[n] * scale - parts[n] * along).astype(BF)
                B[at, cut] = (B[at, cut].astype(F32) + by_h.astype(F32)).astype(BF)

        loop(16, norm_back)

    sum_tick(19, bufs)
    phase_nback()
    sum_tick(20, bufs)
    def kept_tile(number_of, e):
        return (
            copy(silus.at[number_of], F.at[e], tiles.at[0, e]),
            copy(slopes.at[number_of], F.at[2 + e], tiles.at[1, e]),
        )

    tall_quarter(0, 0, 0)
    for one in kept_tile(0, 0):
        one.start()
    tall_gradient(0, 24, 21, (0, 1, 3, 5, 7), 1, lambda: None)

    copy(a0, A, load.at[1]).wait()
    def phase_l0():
        def layer_0(q):
            b = q % 2
            loaded(b)

            @pl.when(q < 3)
            def _():
                tall_quarter(0, q + 1, 1 - b)

            def tile(i):
                sum_at(i != 1, 26 + 5 * q + i // 2 + i // 3)
                n, m, e = i // 2, i % 2, i % 2
                number_of = 4 * q + i
                for one in kept_tile(number_of, e):
                    one.wait()

                @pl.when(number_of < 15)
                def _():
                    for one in kept_tile(number_of + 1, 1 - e):
                        one.start()

                for part in range(2):
                    here = pl.ds(512 * part, 512)
                    there = pl.ds(pl.multiple_of(m * 1024 + 512 * part, 512), 512)
                    by_act = dot(B[there], W[b, half(n)], NT).astype(BF).astype(F32)
                    D[1, there, half(n)] = (by_act * F[e, here]).astype(BF)
                    D[0, there, half(n)] = (by_act * F[2 + e, here]).astype(BF)

            loop(4, tile)
            def part(i):
                sum_at(jnp.logical_or(jnp.logical_or(i == 1, i == 2), jnp.logical_and(q == 3, i == 3)), 28 + 5 * q + i)
                keep_wide(own, 32 + 4 * q + i, dot(A[...], D[i // 2, :, half(i % 2)], TN), c)

            loop(4, part)

        loop(4, layer_0)

    phase_l0()
    loop(SUM_AT[-1] + 1, lambda t: sum_tick(CHUNKS - 1 + t, bufs))
    all_squares(squares, total, box, last)
    copy(pack, pack, glocal.at[0]).wait()


def stepped(x, dy, weights):
    block, hbm, shape = (4, 32, 128), pl.BlockSpec(memory_space=pl.ANY), jax.ShapeDtypeStruct
    results = pl.pallas_call(
        step_kernel,
        name="step",
        out_shape=[shape((1, 1), F32)]
        + [shape(w.shape, BF) for w in weights]
        + [
            shape((CHUNKS, 2, 2, 4, 2) + block, BF),
            shape((2, 4, 2048, 1024), BF),
            shape((16, 1024, 512), F32),
            shape((16, 1024, 512), F32),
            shape((16, 1024, 512), BF),
            shape((2048, 1024), BF),
            shape((2048, 1024), BF),
        ],
        in_specs=[hbm] * 5,
        out_specs=[pl.BlockSpec(memory_space=pltpu.SMEM)] + [hbm] * 10,
        scratch_shapes=[
            pltpu.VMEM((2048, 1024), BF),
            pltpu.VMEM((2048, 1024), BF),
            pltpu.VMEM((2, 2048, 1024), BF),
            pltpu.VMEM((2, 1024, 1024), BF),
            pltpu.VMEM((4, 1024, 512), F32),
            pltpu.VMEM((4, 1024, 512), BF),
            pltpu.VMEM((CHUNKS,) + block, BF),
            pltpu.VMEM((OWN + OTHER, 2, 2, 4) + block, BF),
            pltpu.VMEM((SLOTS, 2, 2, 4) + block, BF),
            pltpu.VMEM((SLOTS, 2, 4) + block, BF),
            pltpu.VMEM((SLOTS, 4) + block, BF),
            pltpu.VMEM((FROMZ, 3, 2) + block, BF),
            pltpu.VMEM((8, 128), F32),
            pltpu.VMEM((12, 8, 128), F32),
            pltpu.SemaphoreType.DMA((CHUNKS, 4)),
            pltpu.SemaphoreType.DMA((5,)),
            pltpu.SemaphoreType.DMA((SLOTS, 6)),
            pltpu.SemaphoreType.DMA((2, 2)),
            pltpu.SemaphoreType.DMA((6,)),
            pltpu.SemaphoreType.DMA((2, 2)),
        ],
        compiler_params=pltpu.CompilerParams(collective_id=0, has_side_effects=True, vmem_limit_bytes=67043328),
    )(x, dy, *weights)
    return results[0], results[1:4]


def solution(mesh):
    def step(x, dy, *arrays):
        weights, m, v = (arrays[i : i + 3] for i in (0, 3, 6))
        squares, mine = stepped(x, dy, weights)
        count = 32 * sum(g.size for g in mine)
        factor = jnp.minimum(1.0, 0.5 * lax.rsqrt(squares[0, 0] / count + 1e-30))
        new = [adamw(w.astype(F32), m, v, g.astype(F32) * factor) for w, m, v, g in zip(weights, m, v, mine, strict=True)]
        return tuple(one[which] for which in range(3) for one in new)

    states, cut = P(("rep", "dp"), None, None), P(None, "dp", None)
    return jax.shard_map(
        step,
        mesh=mesh,
        in_specs=(states, states) + (cut,) * 9,
        out_specs=(P("rep", "dp", None),) * 9,
        check_vma=False,
    )
```
